8 devices in a mesh: pairs: 1 (over z), cols: 2 (over y), rows: 4 (over x, core).
Axes of the slice: x: 2, y: 2, z: 1, core: 2. Of those that a mesh axis runs over, the one named last changes fastest.
Arguments:
- C1: float32 [3072, 3072], P(('pairs', 'rows'), 'cols')
- C2: float32 [8192, 8192], P(('pairs', 'rows'), 'cols')
- T0: float32 [3072, 8192], P(('pairs', 'rows'), 'cols')
- p: float32 [3072], P(('pairs', 'rows'))
- q: float32 [8192], P(('pairs', 'cols'))
- eps: float32 [8], P('pairs')
Outputs:
- output 1: float32 [3072, 8192], P(('pairs', 'rows'), 'cols')
- output 2: float32 [1], P('pairs')
All inputs are finite; a program needn't handle non-finite values.
Results may differ from the reference program's by a relative error of at most 0.001.
Values are sent between devices in bfloat16 or wider.
A program may use at most 1 GiB of HBM per device.

```python
import jax
import jax.numpy as jnp
from jax import lax

N = 3072
M = 8192
DX = 300
DY = 300
OUTER = 8
SWEEPS = 10
CLUSTERS = 8
PROBE = 256


def cloud_dists(key, count, dim):
    subkeys = jax.random.split(key, 4)
    labels = jax.random.randint(subkeys[0], (count,), 0, CLUSTERS)
    centers = jax.random.normal(subkeys[1], (CLUSTERS, dim), jnp.float32)
    widths = jax.random.uniform(subkeys[2], (CLUSTERS, 1), jnp.float32, 0.2, 0.6)
    points = centers[labels] + widths[labels] * jax.random.normal(subkeys[3], (count, dim), jnp.float32)
    sq_norm = jnp.sum(points * points, axis=1)
    dists = jnp.maximum(sq_norm[:, None] + sq_norm[None, :] - 2.0 * jnp.dot(points, points.T), 0.0)
    dists = 0.5 * (dists + dists.T) * (1.0 - jnp.eye(count, dtype=jnp.float32))
    return points, dists / jnp.max(dists)


def point_features(key, points):
    projection = jax.random.normal(key, (points.shape[1], 4), jnp.float32)
    embedded = jnp.dot(points, projection)
    embedded = embedded - jnp.mean(embedded, axis=0)
    return embedded / jnp.std(embedded, axis=0)


def eps_schedule(key, C1, C2, T0, p, q):
    probe_rows = min(N, PROBE)
    c1_probe = C1[:probe_rows]
    lead_mat = jnp.dot(c1_probe, T0)
    cost_mat = jnp.dot(c1_probe * c1_probe, p)[:, None] + jnp.dot(C2 * C2, q)[None, :] - 2.0 * jnp.dot(lead_mat, C2)
    spread = jnp.mean(jnp.max(cost_mat, axis=1) - jnp.min(cost_mat, axis=1))
    ratios = jax.random.uniform(key, (OUTER,), jnp.float32, 6.0, 14.0)
    return spread / ratios


def setup_inputs(seed: int = 0, part: int = 0) -> dict:
    key = jax.random.fold_in(jax.random.key(seed), part)
    subkeys = jax.random.split(key, 7)
    points_x, C1 = cloud_dists(subkeys[0], N, DX)
    points_y, C2 = cloud_dists(subkeys[1], M, DY)
    p_raw = jax.random.uniform(subkeys[2], (N,), jnp.float32, 0.25, 1.75)
    q_raw = jax.random.uniform(subkeys[3], (M,), jnp.float32, 0.25, 1.75)
    p = p_raw / jnp.sum(p_raw)
    q = q_raw / jnp.sum(q_raw)
    feat_x = point_features(subkeys[4], points_x)
    feat_y = point_features(subkeys[5], points_y)
    tilt_map = 1.0 + 0.8 * jnp.tanh(0.5 * jnp.dot(feat_x, feat_y.T))
    T0 = p[:, None] * q[None, :] * tilt_map
    T0 = T0 / jnp.sum(T0)
    eps = eps_schedule(subkeys[6], C1, C2, T0, p, q)
    return {"C1": C1, "C2": C2, "T0": T0, "p": p, "q": q, "eps": eps}


def reference(C1, C2, T0, p, q, eps):
    c1_half = C1.astype(jnp.bfloat16)
    c2_half = C2.astype(jnp.bfloat16)
    const_c = jnp.dot(C1 * C1, p)[:, None] + jnp.dot(C2 * C2, q)[None, :]

    def cost_of(plan_mat):
        lead_mat = jnp.dot(c1_half, plan_mat.astype(jnp.bfloat16), preferred_element_type=jnp.float32)
        cross_mat = jnp.dot(lead_mat.astype(jnp.bfloat16), c2_half, preferred_element_type=jnp.float32)
        return const_c - 2.0 * cross_mat

    def outer_step(plan_mat, eps_step):
        cost_mat = cost_of(plan_mat)
        kernel = jnp.exp(-(cost_mat - jnp.min(cost_mat, axis=1, keepdims=True)) / eps_step)

        def sweep(sweep_idx, scales):
            row_scale = p / jnp.sum(kernel * scales[1][None, :], axis=1)
            col_scale = q / jnp.sum(kernel * row_scale[:, None], axis=0)
            return row_scale, col_scale

        row_scale, col_scale = lax.fori_loop(0, SWEEPS, sweep, (jnp.ones_like(p), jnp.ones_like(q)))
        return row_scale[:, None] * kernel * col_scale[None, :], eps_step

    plan_mat = lax.scan(outer_step, T0, eps)[0]
    loss_val = jnp.sum(cost_of(plan_mat) * plan_mat)
    return plan_mat, loss_val.reshape(1)
```

```python
import functools

import jax
import jax.numpy as jnp
from jax import lax
from jax.experimental import pallas as pl
from jax.experimental.pallas import tpu as pltpu
from jax.sharding import PartitionSpec as P

SWEEPS = 10
W = 256
AHEAD = 4
RB = 64
LEADS = 4
LANES = 128
SUB = 8
F32 = jnp.float32
BF16 = jnp.bfloat16


def outer_kernel(steps, c1_ref, t0_ref, c2_ref, a_ref, b_ref, p_ref, q_ref, eps_ref, t_out, loss_out,
                 acc, panel, lead, lead_in, c2_own, c2_in, v_ref, r_send, r_in, c_send, c_in, stage,
                 x_send, x_recv, d_send, d_recv, f_send, f_recv, y_send, y_recv,
                 own_sem, in_sem, rs_sem, rr_sem, cs_sem, cr_sem, io_sem, st_sem):
    rows, cols = acc.shape
    chunks = cols // W
    row_at = lax.axis_index("rows")
    col_at = lax.axis_index("cols")
    chip, core = row_at // 2, row_at % 2
    sib = chip * 2 + (1 - core)
    across = (1 - chip) * 2 + core
    diag = (1 - chip) * 2 + (1 - core)
    to_sib, to_across, to_diag, to_col = {"rows": sib}, {"rows": across}, {"rows": diag}, {"cols": 1 - col_at}
    trio = (to_sib, to_across, to_diag)

    barrier = pltpu.get_barrier_semaphore()
    for dev in (*trio, to_col):
        pl.semaphore_signal(barrier, inc=1, device_id=dev)
    pl.semaphore_wait(barrier, 4)

    def rows_of(owner):
        return pl.ds(pl.multiple_of(owner * rows, rows), rows)

    def x_copy(j):
        part = panel.at[j, rows_of(row_at)]
        return pltpu.make_async_remote_copy(part, part, x_send.at[j], x_recv.at[j], device_id=to_across)

    def d_copy(j):
        part = panel.at[j, rows_of(row_at)]
        return pltpu.make_async_remote_copy(part, part, d_send.at[j], d_recv.at[j], device_id=to_sib)

    def f_copy(j):
        part = panel.at[j, rows_of(across)]
        return pltpu.make_async_remote_copy(part, part, f_send.at[j], f_recv.at[j], device_id=to_sib)

    def y_copy(j):
        return pltpu.make_async_remote_copy(lead.at[j % LEADS], lead_in.at[j], y_send.at[j], y_recv.at[j], device_id=to_col)

    def c2_copy(owner, i, buf, sem):
        src = c2_ref.at[pl.ds(pl.multiple_of(owner * cols + i * W, W), W)]
        return pltpu.make_async_copy(src, buf.at[i % 2], sem.at[i % 2])

    def own_copy(i):
        return c2_copy(col_at, i, c2_own, own_sem)

    def in_copy(i):
        return c2_copy(1 - col_at, i, c2_in, in_sem)

    def add_product(left, right, first):
        tile = 512

        def body(n, _):
            at = pl.ds(pl.multiple_of(n * tile, tile), tile)
            prod = jnp.dot(left[...], right[:, at], preferred_element_type=F32)
            if first:
                acc[:, at] = prod
            else:
                acc[:, at] = acc[:, at] + prod
            return 0
        lax.fori_loop(0, cols // tile, body, 0)

    lane = lax.broadcasted_iota(jnp.int32, (SUB, LANES), 1)

    def unpack(packed, g):
        return jnp.sum(jnp.where(lane == g, packed, 0.0), axis=1, keepdims=True)

    def pack(packed, col, g):
        return jnp.where(lane == g, col, packed)

    def lanes(t):
        return slice(t * LANES, (t + 1) * LANES)

    tiles = cols // LANES
    per = RB // SUB
    blocks = rows // RB

    def row_exchange(value, slot, combine):
        r_send[slot] = value
        copy = pltpu.make_async_remote_copy(r_send.at[slot], r_in.at[slot], rs_sem.at[slot], rr_sem.at[slot], device_id=to_col)
        copy.start()
        copy.wait()
        return combine(value, r_in[slot])

    def cost():
        def issue(j, _):
            x_copy(j).start()
            d_copy(j).start()
            return 0
        lax.fori_loop(0, AHEAD, issue, 0)
        for i in range(2):
            own_copy(i).start()
            in_copy(i).start()

        def own_part(i, first):
            own_copy(i).wait()
            add_product(lead.at[i % LEADS], c2_own.at[i % 2], first)

            @pl.when(i + 2 < chunks)
            def _():
                own_copy(i + 2).start()

        def step(j, _):
            @pl.when(j < chunks)
            def _():
                x_copy(j).wait_recv()
                f_copy(j).start()

                @pl.when(j + AHEAD < chunks)
                def _():
                    issue(j + AHEAD, 0)

            @pl.when(j == 1)
            def _():
                own_part(0, True)

            @pl.when((j > 1) & (j <= chunks))
            def _():
                own_part(j - 1, False)

            @pl.when(j < chunks)
            def _():
                d_copy(j).wait_recv()
                f_copy(j).wait_recv()

                @pl.when(j >= LEADS)
                def _():
                    y_copy(j - LEADS).wait_send()
                lead[j % LEADS] = jnp.dot(c1_ref[...], panel[j], preferred_element_type=F32).astype(BF16)
                y_copy(j).start()

            @pl.when(j >= 2)
            def _():
                i = j - 2
                y_copy(i).wait_recv()
                in_copy(i).wait()
                add_product(lead_in.at[i], c2_in.at[i % 2], False)

                @pl.when(i + 2 < chunks)
                def _():
                    in_copy(i + 2).start()
            return 0
        lax.fori_loop(0, chunks + 2, step, 0)

        def drain(j, _):
            x_copy(j).wait_send()
            d_copy(j).wait_send()
            f_copy(j).wait_send()
            return 0
        lax.fori_loop(0, chunks, drain, 0)
        for j in range(chunks - LEADS, chunks):
            y_copy(j).wait_send()

    def cost_min():
        def body(i, packed):
            at = pl.ds(pl.multiple_of(i * RB, RB), RB)
            a_rep = jnp.concatenate([jnp.broadcast_to(unpack(a_ref[...], i * per + k), (SUB, LANES)) for k in range(per)], axis=0)
            low = None
            for t in range(tiles):
                val = (a_rep + b_ref[:, lanes(t)]) - 2.0 * acc[at, lanes(t)]
                acc[at, lanes(t)] = val
                low = val if low is None else jnp.minimum(low, val)
            low = jnp.min(low, axis=1, keepdims=True)
            for k in range(per):
                packed = pack(packed, low[k * SUB:(k + 1) * SUB], i * per + k)
            return packed
        return lax.fori_loop(0, blocks, body, jnp.zeros((SUB, LANES), F32))

    def gibbs(low, scale):
        def body(i, packed):
            at = pl.ds(pl.multiple_of(i * RB, RB), RB)
            low_rep = jnp.concatenate([jnp.broadcast_to(unpack(low, i * per + k), (SUB, LANES)) for k in range(per)], axis=0)
            total = None
            for t in range(tiles):
                val = jnp.exp((low_rep - acc[at, lanes(t)]) * scale)
                acc[at, lanes(t)] = val
                total = val if total is None else total + val
            total = jnp.sum(total, axis=1, keepdims=True)
            for k in range(per):
                packed = pack(packed, total[k * SUB:(k + 1) * SUB], i * per + k)
            return packed
        return lax.fori_loop(0, blocks, body, jnp.ones((SUB, LANES), F32))

    def row_sums():
        def body(i, packed):
            at = pl.ds(pl.multiple_of(i * RB, RB), RB)
            total = None
            for t in range(tiles):
                val = acc[at, lanes(t)] * v_ref[:, lanes(t)]
                total = val if total is None else total + val
            total = jnp.sum(total, axis=1, keepdims=True)
            for k in range(per):
                packed = pack(packed, total[k * SUB:(k + 1) * SUB], i * per + k)
            return packed
        return lax.fori_loop(0, blocks, body, jnp.ones((SUB, LANES), F32))

    def col_sums(u, slot):
        def body(i, sums):
            reps = [jnp.broadcast_to(unpack(u, i * per + k), (SUB, LANES)) for k in range(per)]
            out = []
            for t in range(tiles):
                val = sums[t]
                for k in range(per):
                    val = val + acc[pl.ds(pl.multiple_of(i * RB + k * SUB, SUB), SUB), lanes(t)] * reps[k]
                out.append(val)
            return tuple(out)
        sums = lax.fori_loop(0, blocks, body, tuple(jnp.zeros((SUB, LANES), F32) for _ in range(tiles)))
        for t in range(tiles):
            c_send[slot, :, lanes(t)] = jnp.sum(sums[t], axis=0, keepdims=True)

    def col_update(u, slot):
        col_sums(u, slot)
        copies = [
            pltpu.make_async_remote_copy(c_send.at[slot], c_in.at[slot, n], cs_sem.at[slot, n], cr_sem.at[slot, n], device_id=dev)
            for n, dev in enumerate(trio)
        ]
        for copy in copies:
            copy.start()
        for copy in copies:
            copy.wait()
        v_ref[...] = q_ref[...] / ((c_send[slot] + c_in[slot, 0]) + (c_in[slot, 1] + c_in[slot, 2]))

    def make_plan(u):
        def body(i, _):
            at = pl.ds(pl.multiple_of(i * RB, RB), RB)
            u_rep = jnp.concatenate([jnp.broadcast_to(unpack(u, i * per + k), (SUB, LANES)) for k in range(per)], axis=0)
            for t in range(tiles):
                val = (u_rep * acc[at, lanes(t)]) * v_ref[:, lanes(t)]
                acc[at, lanes(t)] = val
                half = (t * LANES) % W
                panel[t * LANES // W, pl.ds(pl.multiple_of(row_at * rows + i * RB, RB), RB), half:half + LANES] = val.astype(BF16)
            return 0
        lax.fori_loop(0, blocks, body, 0)

    def sinkhorn(r):
        low = row_exchange(cost_min(), 2, jnp.minimum)
        first = gibbs(low, 1.0 / eps_ref[r])
        u = p_ref[...] / row_exchange(first, 0, jnp.add)
        col_update(u, 0)

        def sweep(s, u):
            slot = s % 2
            u = p_ref[...] / row_exchange(row_sums(), slot, jnp.add)
            col_update(u, slot)
            return u
        u = lax.fori_loop(1, SWEEPS, sweep, u)
        make_plan(u)

    def stage_copy(i):
        return pltpu.make_async_copy(t_out.at[pl.ds(pl.multiple_of(i * SUB, SUB), SUB)], stage.at[i % 2], st_sem.at[i % 2])

    def loss():
        groups = rows // SUB
        stage_copy(0).start()

        def body(g, total):
            @pl.when(g + 1 < groups)
            def _():
                stage_copy(g + 1).start()
            stage_copy(g).wait()
            at = pl.ds(pl.multiple_of(g * SUB, SUB), SUB)
            a_rep = jnp.broadcast_to(unpack(a_ref[...], g), (SUB, LANES))
            part = None
            for t in range(tiles):
                val = ((a_rep + b_ref[:, lanes(t)]) - 2.0 * acc[at, lanes(t)]) * stage[g % 2, :, lanes(t)]
                part = val if part is None else part + val
            return total + part
        loss_out[...] = lax.fori_loop(0, groups, body, jnp.zeros((SUB, LANES), F32))

    first_plan = pltpu.make_async_copy(t0_ref, panel.at[:, rows_of(row_at)], io_sem)
    first_plan.start()
    first_plan.wait()
    plan_out = pltpu.make_async_copy(acc, t_out, io_sem)

    def outer(r, _):
        cost()

        @pl.when(r < steps)
        def _():
            sinkhorn(r)

        @pl.when(r == steps - 1)
        def _():
            plan_out.start()
            plan_out.wait()
        return 0
    lax.fori_loop(0, steps + 1, outer, 0)
    loss()


def packed_rows(vec):
    groups = vec.shape[0] // SUB
    return jnp.pad(vec.reshape(groups, SUB).T, ((0, 0), (0, LANES - groups)), constant_values=1.0)


def solution(mesh):
    grid_spec = P(("pairs", "rows"), "cols")

    def local_fn(c1_blk, c2_blk, t0_blk, p_blk, q_blk, eps_blk):
        col_pos = lax.axis_index("cols")
        row_pos = lax.axis_index("rows")
        c1_width = c1_blk.shape[1]
        c2_height = c2_blk.shape[0]
        rows, cols = t0_blk.shape
        chunks = cols // W
        steps = eps_blk.shape[0]
        p_full = lax.all_gather(p_blk, "rows", tiled=True)
        q_full = lax.all_gather(q_blk, "cols", tiled=True)
        p_piece = lax.dynamic_slice_in_dim(p_full, col_pos * c1_width, c1_width)
        q_piece = lax.dynamic_slice_in_dim(q_full, row_pos * c2_height, c2_height)
        row_term = lax.psum(jnp.sum(c1_blk * c1_blk * p_piece[None, :], axis=1), "cols")
        col_term = lax.psum(jnp.sum(c2_blk * c2_blk * q_piece[:, None], axis=0), "rows")
        c1_panel = lax.all_gather(c1_blk.astype(BF16), "cols", axis=1, tiled=True)
        c2_panel = lax.all_gather(c2_blk.astype(BF16), "rows", axis=0, tiled=True)
        t0_chunks = t0_blk.astype(BF16).reshape(rows, chunks, W).transpose(1, 0, 2)

        vmem = pl.BlockSpec(memory_space=pltpu.VMEM)
        smem = pl.BlockSpec(memory_space=pltpu.SMEM)
        hbm = pl.BlockSpec(memory_space=pl.ANY)
        dma = pltpu.SemaphoreType.DMA
        plan, loss_part = pl.pallas_call(
            functools.partial(outer_kernel, steps),
            out_shape=(jax.ShapeDtypeStruct((rows, cols), F32), jax.ShapeDtypeStruct((SUB, LANES), F32)),
            in_specs=[vmem, hbm, hbm, vmem, vmem, vmem, vmem, smem],
            out_specs=(hbm, vmem),
            scratch_shapes=[
                pltpu.VMEM((rows, cols), F32),
                pltpu.VMEM((chunks, 4 * rows, W), BF16),
                pltpu.VMEM((LEADS, rows, W), BF16),
                pltpu.VMEM((chunks, rows, W), BF16),
                pltpu.VMEM((2, W, cols), BF16),
                pltpu.VMEM((2, W, cols), BF16),
                pltpu.VMEM((1, cols), F32),
                pltpu.VMEM((3, SUB, LANES), F32),
                pltpu.VMEM((3, SUB, LANES), F32),
                pltpu.VMEM((2, 1, cols), F32),
                pltpu.VMEM((2, 3, 1, cols), F32),
                pltpu.VMEM((2, SUB, cols), F32),
                *[dma((chunks,))] * 8,
                dma((2,)), dma((2,)), dma((3,)), dma((3,)), dma((2, 3)), dma((2, 3)),
                dma, dma((2,)),
            ],
            compiler_params=pltpu.CompilerParams(collective_id=0, has_side_effects=True, vmem_limit_bytes=67043328),
        )(c1_panel, t0_chunks, c2_panel, packed_rows(row_term), col_term[None], packed_rows(p_blk), q_blk[None], eps_blk)
        return plan, lax.psum(jnp.sum(loss_part), ("rows", "cols")).reshape(1)

    return jax.shard_map(local_fn, mesh=mesh, in_specs=(grid_spec, grid_spec, grid_spec, P(("pairs", "rows")), P(("pairs", "cols")), P("pairs")), out_specs=(grid_spec, P("pairs")), check_vma=False)
```

```python
import functools

import jax
import jax.numpy as jnp
from jax import lax
from jax.experimental import pallas as pl
from jax.experimental.pallas import tpu as pltpu
from jax.sharding import PartitionSpec as P

SWEEPS = 10
W = 256
AHEAD = 4
RB = 64
HALF = 8
LANES = 128
SUB = 8
F32 = jnp.float32
BF16 = jnp.bfloat16


def outer_kernel(steps, c1_blk, t0_ref, c2_blk, a_ref, b_part, p_ref, q_ref, eps_ref, t_out, loss_out, c2_ref, c2_turn,
                 acc, panel, c1_ref, lead_in, c2_own, c2_in, turn_in, turn_out, b_ref, v_ref, a_rep, u_rep, part, c_part,
                 m_send, m_in, r_send, r_in, c_send, c_in, stage,
                 x_send, x_recv, d_send, d_recv, f_send, f_recv, y_send, y_recv,
                 own_sem, in_sem, ms_sem, mr_sem, rs_sem, rr_sem, cs_sem, cr_sem, io_sem, st_sem,
                 xs_sem, xr_sem, ts_sem, tr_sem, fs_sem, fr_sem, us_sem, ur_sem, bs_sem, br_sem, os_sem, or_sem, turn_sem):
    rows, cols = acc.shape
    chunks = cols // W
    row_at = lax.axis_index("rows")
    col_at = lax.axis_index("cols")
    chip, core = row_at // 2, row_at % 2
    sib = chip * 2 + (1 - core)
    across = (1 - chip) * 2 + core
    diag = (1 - chip) * 2 + (1 - core)
    to_sib, to_across, to_diag, to_col = {"rows": sib}, {"rows": across}, {"rows": diag}, {"cols": 1 - col_at}
    trio = (to_sib, to_across, to_diag)

    barrier = pltpu.get_barrier_semaphore()
    for dev in (*trio, to_col):
        pl.semaphore_signal(barrier, inc=1, device_id=dev)
    pl.semaphore_wait(barrier, 4)

    def rows_of(owner):
        return pl.ds(pl.multiple_of(owner * rows, rows), rows)

    def lead_at(j):
        return panel.at[j, rows_of(sib)]

    def x_copy(j):
        part = panel.at[j, rows_of(row_at)]
        return pltpu.make_async_remote_copy(part, part, x_send.at[j], x_recv.at[j], device_id=to_across)

    def d_copy(j):
        part = panel.at[j, rows_of(row_at)]
        return pltpu.make_async_remote_copy(part, part, d_send.at[j], d_recv.at[j], device_id=to_sib)

    def f_copy(j):
        part = panel.at[j, rows_of(across)]
        return pltpu.make_async_remote_copy(part, part, f_send.at[j], f_recv.at[j], device_id=to_sib)

    def y_copy(j):
        return pltpu.make_async_remote_copy(lead_at(j), lead_in.at[j], y_send.at[j], y_recv.at[j], device_id=to_col)

    held = c2_blk.shape[0]
    here = held // W

    def wide(n):
        return pl.ds(pl.multiple_of(n * W, W), W)

    def c2_start(owner, i, buf, sem):
        block = owner * (chunks // here) + i // here

        @pl.when(block == row_at)
        def _():
            pltpu.make_async_copy(c2_blk.at[wide(i % here)], buf.at[i % 2], sem.at[i % 2]).start()

        @pl.when(block != row_at)
        def _():
            for n in range(chunks):
                pltpu.make_async_copy(c2_ref.at[n, wide(owner * chunks + i)], buf.at[i % 2, :, n * W:(n + 1) * W], sem.at[i % 2]).start()

    def c2_wait(i, buf, sem):
        pltpu.make_async_copy(c2_blk.at[0:W], buf.at[i % 2], sem.at[i % 2]).wait()

    def add_product(left, right, first):
        tile = 512

        def body(n, _):
            at = pl.ds(pl.multiple_of(n * tile, tile), tile)
            prod = jnp.dot(left[...], right[:, at], preferred_element_type=F32)
            if first:
                acc[:, at] = prod
            else:
                acc[:, at] = acc[:, at] + prod
            return 0
        lax.fori_loop(0, cols // tile, body, 0)

    lane = lax.broadcasted_iota(jnp.int32, (SUB, LANES), 1)

    def lanes(t):
        return slice(t * LANES, (t + 1) * LANES)

    tiles = cols // LANES
    per = RB // SUB
    blocks = rows // RB
    groups = rows // SUB

    def issue(j):
        x_copy(j).start()
        d_copy(j).start()

    def product(owner, i, left, buf, sem, first=False):
        c2_wait(i, buf, sem)
        add_product(left, buf.at[i % 2], first)

        @pl.when(i + 2 < chunks)
        def _():
            c2_start(owner, i + 2, buf, sem)

    def take_chunk(j):
        x_copy(j).wait_recv()
        f_copy(j).start()

        @pl.when(j + AHEAD < chunks)
        def _():
            issue(j + AHEAD)

    def form_lead(j):
        d_copy(j).wait_recv()
        f_copy(j).wait_recv()
        panel[j, rows_of(sib)] = jnp.dot(c1_ref[...], panel[j], preferred_element_type=F32).astype(BF16)
        y_copy(j).start()

    def drain_chunks():
        def drain(j, _):
            x_copy(j).wait_send()
            d_copy(j).wait_send()
            f_copy(j).wait_send()
            y_copy(j).wait_send()
            return 0
        lax.fori_loop(0, chunks, drain, 0)

    def cost():
        for i in range(2):
            c2_start(col_at, i, c2_own, own_sem)
            c2_start(1 - col_at, i, c2_in, in_sem)

        def step(j, _):
            @pl.when(j < chunks)
            def _():
                take_chunk(j)

            @pl.when(j == 1)
            def _():
                product(col_at, 0, lead_at(0), c2_own, own_sem, True)

            @pl.when((j > 1) & (j <= chunks))
            def _():
                product(col_at, j - 1, lead_at(j - 1), c2_own, own_sem)

            @pl.when(j < chunks)
            def _():
                form_lead(j)

            @pl.when(j >= 2)
            def _():
                y_copy(j - 2).wait_recv()
                product(1 - col_at, j - 2, lead_in.at[j - 2], c2_in, in_sem)
            return 0
        lax.fori_loop(0, chunks + 2, step, 0)
        drain_chunks()

    far = 1 - chip

    def quad_rows(base, k):
        return pl.ds(pl.multiple_of(base + k * W, W), W)

    def many(ref, count):
        return ref.at[pl.ds(0, count), pl.ds(0, W)]

    def own_piece(n, m):
        return c2_blk.at[wide(m), wide(n)]

    def sends(src, dst, dst_base, k, m, offsets, sem_s, sem_r, dev):
        for d in offsets:
            n = (k + d) % chunks
            to = dst.at[n, quad_rows(dst_base, m)]
            pltpu.make_async_remote_copy(own_piece(n, m) if src is None else src.at[n, quad_rows(dst_base, m)], to,
                                         sem_s.at[m], sem_r.at[m], device_id=dev).start()

    def group(m, count, sem_s, sem_r, dev):
        return pltpu.make_async_remote_copy(many(c2_ref, count), many(c2_ref, count), sem_s.at[m], sem_r.at[m], device_id=dev)

    straight, turned = range(HALF + 1), range(1, HALF)
    across_base, turn_base = across * held, core * held

    def row_send(m):
        k = core * here + m
        sends(None, c2_ref, row_at * held, k, m, straight, xs_sem, xr_sem, to_across)
        sends(None, c2_turn, turn_base, k, m, turned, ts_sem, tr_sem, to_col)

    def row_forward(m):
        k = core * here + m
        group(m, HALF + 1, xs_sem, xr_sem, to_across).wait_recv()
        sends(c2_ref, c2_ref, across_base, k, m, straight, fs_sem, fr_sem, to_sib)
        group(m, HALF - 1, ts_sem, tr_sem, to_col).wait_recv()
        sends(c2_turn, c2_turn, turn_base, k, m, turned, us_sem, ur_sem, to_sib)

    def row_turn(k):
        def load(src, base):
            for d in turned:
                pltpu.make_async_copy(src.at[(k + d) % chunks, quad_rows(base, k)], turn_in.at[d - 1], turn_sem.at[0]).start()

        @pl.when(chip == col_at)
        def _():
            load(c2_turn, 0)

        @pl.when(chip != col_at)
        def _():
            load(c2_ref, far * cols)
        pltpu.make_async_copy(many(c2_ref, HALF - 1), turn_in, turn_sem.at[0]).wait()
        for d in turned:
            turn_out[d - 1] = turn_in[d - 1].T
        for d in turned:
            pltpu.make_async_copy(turn_out.at[d - 1], c2_ref.at[k, quad_rows(far * cols, (k + d) % chunks)], turn_sem.at[1]).start()
        pltpu.make_async_copy(turn_out, many(c2_ref, HALF - 1), turn_sem.at[1]).wait()

    def first_cost(own_block, c1_copy):
        own_block.wait_recv()
        for i in range(2):
            c2_start(chip, i, c2_own, own_sem)

        def step(j, _):
            @pl.when((j < chunks) & (j % 2 == 0))
            def _():
                row_send(j // 2)

            @pl.when(j < chunks)
            def _():
                take_chunk(j)

            @pl.when((j == 1) & (chip == col_at))
            def _():
                product(chip, 0, lead_at(0), c2_own, own_sem, True)

            @pl.when((j > 1) & (j <= chunks) & (chip == col_at))
            def _():
                product(chip, j - 1, lead_at(j - 1), c2_own, own_sem)

            @pl.when(j == 0)
            def _():
                c1_copy.wait_recv()

            @pl.when(j < chunks)
            def _():
                form_lead(j)

            @pl.when(j >= 2)
            def _():
                y_copy(j - 2).wait_recv()

            @pl.when((j == 2) & (chip != col_at))
            def _():
                product(chip, 0, lead_in.at[0], c2_own, own_sem, True)

            @pl.when((j > 2) & (chip != col_at))
            def _():
                product(chip, j - 2, lead_in.at[j - 2], c2_own, own_sem)

            @pl.when((j > 2) & (j % 2 == 1))
            def _():
                m = (j - 3) // 2
                row_forward(m)
                row_turn(core * here + m)
                group(m, HALF + 1, fs_sem, fr_sem, to_sib).wait_recv()
                group(m, HALF - 1, us_sem, ur_sem, to_sib).wait_recv()
                row_turn((1 - core) * here + m)
            return 0
        lax.fori_loop(0, chunks + 2, step, 0)

        for i in range(2):
            c2_start(far, i, c2_in, in_sem)

        def rest(i, _):
            @pl.when(chip == col_at)
            def _():
                product(far, i, lead_in.at[i], c2_in, in_sem)

            @pl.when(chip != col_at)
            def _():
                product(far, i, lead_at(i), c2_in, in_sem)
            return 0
        lax.fori_loop(0, chunks, rest, 0)
        drain_chunks()
        own_block.wait_send()
        c1_copy.wait_send()

        def sent_rows(m, _):
            group(m, HALF + 1, xs_sem, xr_sem, to_across).wait_send()
            group(m, HALF - 1, ts_sem, tr_sem, to_col).wait_send()
            group(m, HALF + 1, fs_sem, fr_sem, to_sib).wait_send()
            group(m, HALF - 1, us_sem, ur_sem, to_sib).wait_send()
            return 0
        lax.fori_loop(0, here, sent_rows, 0)

    def spread(packed, out, groups):
        for g in groups:
            val = jnp.sum(jnp.where(lane == g, packed, 0.0), axis=1, keepdims=True)
            out[g * SUB:(g + 1) * SUB] = jnp.broadcast_to(val, (SUB, LANES))

    def gather_rows(reduce, groups):
        packed = jnp.ones((SUB, LANES), F32)
        for g in groups:
            packed = jnp.where(lane == g, reduce(part[g * SUB:(g + 1) * SUB], axis=1, keepdims=True), packed)
        return packed

    def block_at(i):
        return pl.ds(pl.multiple_of(i * RB, RB), RB)

    def cost_min():
        def body(i, _):
            at = block_at(i)
            a_rows = a_rep[at]
            low = None
            for t in range(tiles):
                val = (a_rows + b_ref[:, lanes(t)]) - 2.0 * acc[at, lanes(t)]
                acc[at, lanes(t)] = val
                low = val if low is None else jnp.minimum(low, val)
            part[at] = low
            return 0
        lax.fori_loop(0, blocks, body, 0)
        m_send[...] = gather_rows(jnp.min, range(groups))
        copy = pltpu.make_async_remote_copy(m_send, m_in, ms_sem, mr_sem, device_id=to_col)
        copy.start()
        copy.wait()
        spread(jnp.minimum(m_send[...], m_in[...]), u_rep, range(groups))

    def gibbs(scale):
        def body(i, _):
            at = block_at(i)
            low = u_rep[at]
            total = None
            for t in range(tiles):
                val = jnp.exp((low - acc[at, lanes(t)]) * scale)
                acc[at, lanes(t)] = val
                total = val if total is None else total + val
            part[at] = total
            return 0
        lax.fori_loop(0, blocks, body, 0)

    def row_pass(first_block, last_block, half):
        def body(i, _):
            at = block_at(i)
            total = part[at] if half else None
            for t in range(half * tiles // 2, (half + 1) * tiles // 2):
                val = acc[at, lanes(t)] * v_ref[:, lanes(t)]
                total = val if total is None else total + val
            part[at] = total
            return 0
        lax.fori_loop(first_block, last_block, body, 0)

    def col_pass(first_block, last_block, half, first):
        mine = range(half * tiles // 2, (half + 1) * tiles // 2)

        def body(i, sums):
            reps = [u_rep[pl.ds(pl.multiple_of(i * RB + k * SUB, SUB), SUB)] for k in range(per)]
            out = []
            for t, val in zip(mine, sums):
                for k in range(per):
                    val = val + acc[pl.ds(pl.multiple_of(i * RB + k * SUB, SUB), SUB), lanes(t)] * reps[k]
                out.append(val)
            return tuple(out)
        start = tuple(jnp.zeros((SUB, LANES), F32) if first else c_part[:, lanes(t)] for t in mine)
        return lax.fori_loop(first_block, last_block, body, start)

    def r_copy(slot, half):
        return pltpu.make_async_remote_copy(r_send.at[slot, half], r_in.at[slot, half], rs_sem.at[slot, half], rr_sem.at[slot, half], device_id=to_col)

    def c_copies(slot, half):
        return [
            pltpu.make_async_remote_copy(c_send.at[slot, half], c_in.at[slot, half, n], cs_sem.at[slot, half, n], cr_sem.at[slot, half, n], device_id=dev)
            for n, dev in enumerate(trio)
        ]

    mid_group, mid_block, mid_col = groups // 2, blocks // 2, cols // 2

    def send_rows(slot, half):
        r_send[slot, half] = gather_rows(jnp.sum, range(half * mid_group, (half + 1) * mid_group))
        r_copy(slot, half).start()

    def take_rows(slot, half):
        r_copy(slot, half).wait_recv()
        u = p_ref[...] / (r_send[slot, half] + r_in[slot, half])
        spread(u, u_rep, range(half * mid_group, (half + 1) * mid_group))

    def send_cols(slot, half, sums):
        for t, val in enumerate(sums):
            c_send[slot, half, :, lanes(t)] = jnp.sum(val, axis=0, keepdims=True)
        for copy in c_copies(slot, half):
            copy.start()

    def take_cols(slot, half):
        for copy in c_copies(slot, half):
            copy.wait_recv()
        at = slice(half * mid_col, (half + 1) * mid_col)
        total = (c_send[slot, half] + c_in[slot, half, 0]) + (c_in[slot, half, 1] + c_in[slot, half, 2])
        v_ref[:, at] = q_ref[:, at] / total

    def sent(slot):
        for half in range(2):
            r_copy(slot, half).wait_send()
            for copy in c_copies(slot, half):
                copy.wait_send()

    def make_plan():
        def chunk(j, _):
            def body(i, _):
                at = block_at(i)
                for t in range(W // LANES):
                    where = pl.ds(pl.multiple_of(j * W + t * LANES, LANES), LANES)
                    val = (u_rep[at] * acc[at, where]) * v_ref[:, where]
                    acc[at, where] = val
                    panel[j, pl.ds(pl.multiple_of(row_at * rows + i * RB, RB), RB), lanes(t)] = val.astype(BF16)
                return 0
            lax.fori_loop(0, blocks, body, 0)

            @pl.when(j < AHEAD)
            def _():
                issue(j)
            return 0
        lax.fori_loop(0, chunks, chunk, 0)

    def sinkhorn(r):
        cost_min()
        gibbs(1.0 / eps_ref[r])

        def sweep(s, _):
            slot = s % 2

            @pl.when(s == 0)
            def _():
                send_rows(slot, 0)
                send_rows(slot, 1)

            @pl.when(s > 0)
            def _():
                take_cols(1 - slot, 0)
                row_pass(0, blocks, 0)
                take_cols(1 - slot, 1)
                row_pass(0, mid_block, 1)
                send_rows(slot, 0)
                row_pass(mid_block, blocks, 1)
                send_rows(slot, 1)

            take_rows(slot, 0)
            for half in range(2):
                for t, val in enumerate(col_pass(0, mid_block, half, True)):
                    c_part[:, lanes(half * tiles // 2 + t)] = val
            take_rows(slot, 1)
            for half in range(2):
                send_cols(slot, half, col_pass(mid_block, blocks, half, False))

            @pl.when(s > 0)
            def _():
                sent(1 - slot)
            return 0
        lax.fori_loop(0, SWEEPS, sweep, 0)
        last = (SWEEPS - 1) % 2
        for half in range(2):
            take_cols(last, half)
        sent(last)
        make_plan()

    def stage_copy(i):
        return pltpu.make_async_copy(t_out.at[pl.ds(pl.multiple_of(i * SUB, SUB), SUB)], stage.at[i % 2], st_sem.at[i % 2])

    def loss():
        stage_copy(0).start()

        def body(g, total):
            @pl.when(g + 1 < groups)
            def _():
                stage_copy(g + 1).start()
            stage_copy(g).wait()
            at = pl.ds(pl.multiple_of(g * SUB, SUB), SUB)
            a_rows = a_rep[at]
            out = None
            for t in range(tiles):
                val = ((a_rows + b_ref[:, lanes(t)]) - 2.0 * acc[at, lanes(t)]) * stage[g % 2, :, lanes(t)]
                out = val if out is None else out + val
            return total + out
        loss_out[...] = lax.fori_loop(0, groups, body, jnp.zeros((SUB, LANES), F32))

    for j in range(chunks):
        pltpu.make_async_copy(t0_ref.at[:, j * W:(j + 1) * W], panel.at[j, rows_of(row_at)], io_sem).start()
    first_plan = pltpu.make_async_copy(panel.at[:, rows_of(row_at)], panel.at[:, rows_of(row_at)], io_sem)
    width = c1_blk.shape[1]
    c1_at = c1_ref.at[:, pl.ds(pl.multiple_of(col_at * width, width), width)]
    c1_here = pltpu.make_async_copy(c1_blk, c1_at, st_sem.at[0])
    c1_here.start()
    c1_copy = pltpu.make_async_remote_copy(c1_blk, c1_at, os_sem, or_sem, device_id=to_col)
    c1_copy.start()
    own_rows = c2_ref.at[:, pl.ds(pl.multiple_of(row_at * held, held), held)]
    own_block = pltpu.make_async_remote_copy(own_rows, own_rows, bs_sem, br_sem, device_id=to_sib)
    for n in range(chunks):
        piece = c2_blk.at[:, n * W:(n + 1) * W]
        pltpu.make_async_remote_copy(piece, own_rows.at[n], bs_sem, br_sem, device_id=to_sib).start()
    first_plan.wait()
    for j in range(AHEAD):
        issue(j)

    m_send[...] = a_ref[...]
    a_copy = pltpu.make_async_remote_copy(m_send, m_in, ms_sem, mr_sem, device_id=to_col)
    a_copy.start()
    for half in range(2):
        c_send[0, half] = b_part[:, half * mid_col:(half + 1) * mid_col]
        for copy in c_copies(0, half):
            copy.start()
    a_copy.wait()
    spread(m_send[...] + m_in[...], a_rep, range(groups))
    for half in range(2):
        for copy in c_copies(0, half):
            copy.wait()
        total = (c_send[0, half] + c_in[0, half, 0]) + (c_in[0, half, 1] + c_in[0, half, 2])
        b_ref[:, half * mid_col:(half + 1) * mid_col] = total
    c1_here.wait()
    plan_out = pltpu.make_async_copy(acc, t_out, io_sem)
    first_cost(own_block, c1_copy)

    def outer(r, _):
        sinkhorn(r)

        @pl.when(r == steps - 1)
        def _():
            plan_out.start()
            plan_out.wait()
        cost()
        return 0
    lax.fori_loop(0, steps, outer, 0)
    loss()


def packed_rows(vec):
    groups = vec.shape[0] // SUB
    return jnp.pad(vec.reshape(groups, SUB).T, ((0, 0), (0, LANES - groups)), constant_values=1.0)


def solution(mesh):
    grid_spec = P(("pairs", "rows"), "cols")

    def local_fn(c1_blk, c2_blk, t0_blk, p_blk, q_blk, eps_blk):
        col_pos = lax.axis_index("cols")
        row_pos = lax.axis_index("rows")
        c1_width = c1_blk.shape[1]
        c2_height = c2_blk.shape[0]
        rows, cols = t0_blk.shape
        chunks = cols // W
        steps = eps_blk.shape[0]
        p_full = lax.all_gather(p_blk, "rows", tiled=True)
        q_full = lax.all_gather(q_blk, "cols", tiled=True)
        p_piece = lax.dynamic_slice_in_dim(p_full, col_pos * c1_width, c1_width)
        q_piece = lax.dynamic_slice_in_dim(q_full, row_pos * c2_height, c2_height)
        row_term = jnp.sum(c1_blk * c1_blk * p_piece[None, :], axis=1)
        col_term = jnp.sum(c2_blk * c2_blk * q_piece[:, None], axis=0)

        vmem = pl.BlockSpec(memory_space=pltpu.VMEM)
        smem = pl.BlockSpec(memory_space=pltpu.SMEM)
        hbm = pl.BlockSpec(memory_space=pl.ANY)
        dma = pltpu.SemaphoreType.DMA
        plan, loss_part, _, _ = pl.pallas_call(
            functools.partial(outer_kernel, steps),
            out_shape=(
                jax.ShapeDtypeStruct((rows, cols), F32), jax.ShapeDtypeStruct((SUB, LANES), F32),
                jax.ShapeDtypeStruct((chunks, 2 * cols, W), BF16), jax.ShapeDtypeStruct((chunks, cols, W), BF16),
            ),
            in_specs=[hbm, hbm, hbm, vmem, vmem, vmem, vmem, smem],
            out_specs=(hbm, vmem, hbm, hbm),
            scratch_shapes=[
                pltpu.VMEM((rows, cols), F32),
                pltpu.VMEM((chunks, 4 * rows, W), BF16),
                pltpu.VMEM((rows, 4 * rows), BF16),
                pltpu.VMEM((chunks, rows, W), BF16),
                pltpu.VMEM((2, W, cols), BF16),
                pltpu.VMEM((2, W, cols), BF16),
                pltpu.VMEM((HALF - 1, W, W), BF16),
                pltpu.VMEM((HALF - 1, W, W), BF16),
                pltpu.VMEM((1, cols), F32),
                pltpu.VMEM((1, cols), F32),
                *[pltpu.VMEM((rows, LANES), F32)] * 3,
                pltpu.VMEM((SUB, cols), F32),
                pltpu.VMEM((SUB, LANES), F32),
                pltpu.VMEM((SUB, LANES), F32),
                pltpu.VMEM((2, 2, SUB, LANES), F32),
                pltpu.VMEM((2, 2, SUB, LANES), F32),
                pltpu.VMEM((2, 2, 1, cols // 2), F32),
                pltpu.VMEM((2, 2, 3, 1, cols // 2), F32),
                pltpu.VMEM((2, SUB, cols), F32),
                *[dma((chunks,))] * 8,
                dma((2,)), dma((2,)), dma, dma, dma((2, 2)), dma((2, 2)), dma((2, 2, 3)), dma((2, 2, 3)),
                dma, dma((2,)),
                *[dma((c2_height // W,))] * 8,
                dma, dma, dma, dma, dma((2,)),
            ],
            compiler_params=pltpu.CompilerParams(collective_id=0, has_side_effects=True, vmem_limit_bytes=67043328),
        )(c1_blk.astype(BF16), t0_blk.astype(BF16), c2_blk.astype(BF16), packed_rows(row_term), col_term[None], packed_rows(p_blk), q_blk[None], eps_blk)
        return plan, lax.psum(jnp.sum(loss_part), ("rows", "cols")).reshape(1)

    return jax.shard_map(local_fn, mesh=mesh, in_specs=(grid_spec, grid_spec, grid_spec, P(("pairs", "rows")), P(("pairs", "cols")), P("pairs")), out_specs=(grid_spec, P("pairs")), check_vma=False)
```

```python
import functools

import jax
import jax.numpy as jnp
from jax import lax
from jax.experimental import pallas as pl
from jax.experimental.pallas import tpu as pltpu
from jax.sharding import PartitionSpec as P

SWEEPS = 10
W = 256
AHEAD = 4
RB = 64
HALF = 8
LANES = 128
SUB = 8
F32 = jnp.float32
BF16 = jnp.bfloat16


def outer_kernel(steps, c1_blk, t0_ref, c2_blk, a_ref, b_part, p_ref, q_ref, eps_ref, t_out, loss_out, c2_ref, c2_turn,
                 acc, panel, c1_ref, lead_in, c2_own, c2_in, turn_in, turn_out, b_ref, v_ref, a_rep, u_rep, part, c_part, f_ref,
                 m_send, m_in, r_send, r_in, c_send, c_in, stage,
                 x_send, x_recv, d_send, d_recv, f_send, f_recv, y_send, y_recv,
                 own_sem, in_sem, ms_sem, mr_sem, rs_sem, rr_sem, cs_sem, cr_sem, io_sem, st_sem,
                 xs_sem, xr_sem, ts_sem, tr_sem, fs_sem, fr_sem, us_sem, ur_sem, bs_sem, br_sem, os_sem, or_sem, turn_sem):
    rows, cols = acc.shape
    chunks = cols // W
    row_at = lax.axis_index("rows")
    col_at = lax.axis_index("cols")
    chip, core = row_at // 2, row_at % 2
    sib = chip * 2 + (1 - core)
    across = (1 - chip) * 2 + core
    diag = (1 - chip) * 2 + (1 - core)
    to_sib, to_across, to_diag, to_col = {"rows": sib}, {"rows": across}, {"rows": diag}, {"cols": 1 - col_at}
    trio = (to_sib, to_across, to_diag)

    barrier = pltpu.get_barrier_semaphore()
    for dev in (*trio, to_col):
        pl.semaphore_signal(barrier, inc=1, device_id=dev)
    pl.semaphore_wait(barrier, 4)

    def rows_of(owner):
        return pl.ds(pl.multiple_of(owner * rows, rows), rows)

    def lead_at(j):
        return panel.at[j, rows_of(sib)]

    last = chunks - 1
    halves = (0, 1)

    def cut(owner, j, half):
        if half is None:
            return panel.at[j, rows_of(owner)], j
        return panel.at[last, rows_of(owner), half * LANES:(half + 1) * LANES], last + half

    def x_copy(j, half=None):
        piece, n = cut(row_at, j, half)
        return pltpu.make_async_remote_copy(piece, piece, x_send.at[n], x_recv.at[n], device_id=to_across)

    def d_copy(j, half=None):
        piece, n = cut(row_at, j, half)
        return pltpu.make_async_remote_copy(piece, piece, d_send.at[n], d_recv.at[n], device_id=to_sib)

    def f_copy(j, half=None):
        piece, n = cut(across, j, half)
        return pltpu.make_async_remote_copy(piece, piece, f_send.at[n], f_recv.at[n], device_id=to_sib)

    def y_copy(j, half=None):
        piece, n = cut(sib, j, half)
        dst = lead_in.at[j] if half is None else lead_in.at[last, :, half * LANES:(half + 1) * LANES]
        return pltpu.make_async_remote_copy(piece, dst, y_send.at[n], y_recv.at[n], device_id=to_col)

    held = c2_blk.shape[0]
    here = held // W

    def wide(n):
        return pl.ds(pl.multiple_of(n * W, W), W)

    def c2_start(owner, i, buf, sem):
        block = owner * (chunks // here) + i // here

        @pl.when(block == row_at)
        def _():
            pltpu.make_async_copy(c2_blk.at[wide(i % here)], buf.at[i % 2], sem.at[i % 2]).start()

        @pl.when(block != row_at)
        def _():
            for n in range(chunks):
                pltpu.make_async_copy(c2_ref.at[n, wide(owner * chunks + i)], buf.at[i % 2, :, n * W:(n + 1) * W], sem.at[i % 2]).start()

    def c2_wait(i, buf, sem):
        pltpu.make_async_copy(c2_blk.at[0:W], buf.at[i % 2], sem.at[i % 2]).wait()

    def add_product(left, right, first):
        tile = 512

        def body(n, _):
            at = pl.ds(pl.multiple_of(n * tile, tile), tile)
            prod = jnp.dot(left[...], right[:, at], preferred_element_type=F32)
            if first:
                acc[:, at] = prod
            else:
                acc[:, at] = acc[:, at] + prod
            return 0
        lax.fori_loop(0, cols // tile, body, 0)

    lane = lax.broadcasted_iota(jnp.int32, (SUB, LANES), 1)

    def lanes(t):
        return slice(t * LANES, (t + 1) * LANES)

    tiles = cols // LANES
    per = RB // SUB
    blocks = rows // RB
    groups = rows // SUB

    def issue(j):
        x_copy(j).start()
        d_copy(j).start()

    def product(owner, i, left, buf, sem, first=False):
        c2_wait(i, buf, sem)
        add_product(left, buf.at[i % 2], first)

        @pl.when(i + 2 < chunks)
        def _():
            c2_start(owner, i + 2, buf, sem)

    def take_chunk(j):
        x_copy(j).wait_recv()
        f_copy(j).start()

        @pl.when(j + AHEAD < last)
        def _():
            issue(j + AHEAD)

        @pl.when(j + AHEAD == last)
        def _():
            for half in halves:
                x_copy(last, half).start()
                d_copy(last, half).start()

    def form_lead(j):
        d_copy(j).wait_recv()
        f_copy(j).wait_recv()
        panel[j, rows_of(sib)] = jnp.dot(c1_ref[...], panel[j], preferred_element_type=F32).astype(BF16)
        y_copy(j).start()

    def last_chunk(between):
        for half, meanwhile in zip(halves, between):
            x_copy(last, half).wait_recv()
            f_copy(last, half).start()
            meanwhile()
            d_copy(last, half).wait_recv()
            f_copy(last, half).wait_recv()
            cols_of = slice(half * LANES, (half + 1) * LANES)
            panel[last, rows_of(sib), cols_of] = jnp.dot(c1_ref[...], panel[last, :, cols_of], preferred_element_type=F32).astype(BF16)
            y_copy(last, half).start()

    def drain_chunks():
        def drain(j, _):
            x_copy(j).wait_send()
            d_copy(j).wait_send()
            f_copy(j).wait_send()
            y_copy(j).wait_send()
            return 0
        lax.fori_loop(0, last, drain, 0)
        for half in halves:
            x_copy(last, half).wait_send()
            d_copy(last, half).wait_send()
            f_copy(last, half).wait_send()
            y_copy(last, half).wait_send()

    def cost():
        for i in range(2):
            c2_start(col_at, i, c2_own, own_sem)
            c2_start(1 - col_at, i, c2_in, in_sem)

        def own_part(i, first=False):
            product(col_at, i, lead_at(i), c2_own, own_sem, first)

        def in_part(i):
            product(1 - col_at, i, lead_in.at[i], c2_in, in_sem)

        def step(j, _):
            take_chunk(j)

            @pl.when(j == 1)
            def _():
                own_part(0, True)

            @pl.when(j > 1)
            def _():
                own_part(j - 1)

            form_lead(j)

            @pl.when(j >= 2)
            def _():
                y_copy(j - 2).wait_recv()
                in_part(j - 2)
            return 0
        lax.fori_loop(0, last, step, 0)

        def tail(i, _):
            y_copy(i).wait_recv()
            in_part(i)
            return 0

        last_chunk((lambda: own_part(last - 1), lambda: tail(last - 2, 0)))
        own_part(last)
        tail(last - 1, 0)
        for half in halves:
            y_copy(last, half).wait_recv()
        in_part(last)
        drain_chunks()

    far = 1 - chip

    def quad_rows(base, k):
        return pl.ds(pl.multiple_of(base + k * W, W), W)

    def many(ref, count):
        return ref.at[pl.ds(0, count), pl.ds(0, W)]

    def own_piece(n, m):
        return c2_blk.at[wide(m), wide(n)]

    def sends(src, dst, dst_base, k, m, offsets, sem_s, sem_r, dev):
        for d in offsets:
            n = (k + d) % chunks
            to = dst.at[n, quad_rows(dst_base, m)]
            pltpu.make_async_remote_copy(own_piece(n, m) if src is None else src.at[n, quad_rows(dst_base, m)], to,
                                         sem_s.at[m], sem_r.at[m], device_id=dev).start()

    def group(m, count, sem_s, sem_r, dev):
        return pltpu.make_async_remote_copy(many(c2_ref, count), many(c2_ref, count), sem_s.at[m], sem_r.at[m], device_id=dev)

    straight, turned = range(HALF + 1), range(1, HALF)
    across_base, turn_base = across * held, core * held

    def row_send(m):
        k = core * here + m
        sends(None, c2_ref, row_at * held, k, m, straight, xs_sem, xr_sem, to_across)
        sends(None, c2_turn, turn_base, k, m, turned, ts_sem, tr_sem, to_col)

    def row_forward(m):
        k = core * here + m
        group(m, HALF + 1, xs_sem, xr_sem, to_across).wait_recv()
        sends(c2_ref, c2_ref, across_base, k, m, straight, fs_sem, fr_sem, to_sib)
        group(m, HALF - 1, ts_sem, tr_sem, to_col).wait_recv()
        sends(c2_turn, c2_turn, turn_base, k, m, turned, us_sem, ur_sem, to_sib)

    def row_turn(k):
        def load(src, base):
            for d in turned:
                pltpu.make_async_copy(src.at[(k + d) % chunks, quad_rows(base, k)], turn_in.at[d - 1], turn_sem.at[0]).start()

        @pl.when(chip == col_at)
        def _():
            load(c2_turn, 0)

        @pl.when(chip != col_at)
        def _():
            load(c2_ref, far * cols)
        pltpu.make_async_copy(many(c2_ref, HALF - 1), turn_in, turn_sem.at[0]).wait()
        for d in turned:
            turn_out[d - 1] = turn_in[d - 1].T
        for d in turned:
            pltpu.make_async_copy(turn_out.at[d - 1], c2_ref.at[k, quad_rows(far * cols, (k + d) % chunks)], turn_sem.at[1]).start()
        pltpu.make_async_copy(turn_out, many(c2_ref, HALF - 1), turn_sem.at[1]).wait()

    def first_cost(own_block, c1_copy):
        own_block.wait_recv()
        for i in range(2):
            c2_start(chip, i, c2_own, own_sem)

        def step(j, _):
            @pl.when((j < chunks) & (j % 2 == 0))
            def _():
                row_send(j // 2)

            @pl.when(j < last)
            def _():
                take_chunk(j)

            @pl.when((j == 1) & (chip == col_at))
            def _():
                product(chip, 0, lead_at(0), c2_own, own_sem, True)

            @pl.when((j > 1) & (j <= chunks) & (chip == col_at))
            def _():
                product(chip, j - 1, lead_at(j - 1), c2_own, own_sem)

            @pl.when(j == 0)
            def _():
                c1_copy.wait_recv()

            @pl.when(j < last)
            def _():
                form_lead(j)

            @pl.when(j == last)
            def _():
                last_chunk((lambda: None,) * 2)

            @pl.when((j >= 2) & (j - 2 < last))
            def _():
                y_copy(j - 2).wait_recv()

            @pl.when(j - 2 == last)
            def _():
                for half in halves:
                    y_copy(last, half).wait_recv()

            @pl.when((j == 2) & (chip != col_at))
            def _():
                product(chip, 0, lead_in.at[0], c2_own, own_sem, True)

            @pl.when((j > 2) & (chip != col_at))
            def _():
                product(chip, j - 2, lead_in.at[j - 2], c2_own, own_sem)

            @pl.when((j > 2) & (j % 2 == 1))
            def _():
                m = (j - 3) // 2
                row_forward(m)
                row_turn(core * here + m)
                group(m, HALF + 1, fs_sem, fr_sem, to_sib).wait_recv()
                group(m, HALF - 1, us_sem, ur_sem, to_sib).wait_recv()
                row_turn((1 - core) * here + m)
            return 0
        lax.fori_loop(0, chunks + 2, step, 0)

        for i in range(2):
            c2_start(far, i, c2_in, in_sem)

        def rest(i, _):
            @pl.when(chip == col_at)
            def _():
                product(far, i, lead_in.at[i], c2_in, in_sem)

            @pl.when(chip != col_at)
            def _():
                product(far, i, lead_at(i), c2_in, in_sem)
            return 0
        lax.fori_loop(0, chunks, rest, 0)
        drain_chunks()
        own_block.wait_send()
        c1_copy.wait_send()

        def sent_rows(m, _):
            group(m, HALF + 1, xs_sem, xr_sem, to_across).wait_send()
            group(m, HALF - 1, ts_sem, tr_sem, to_col).wait_send()
            group(m, HALF + 1, fs_sem, fr_sem, to_sib).wait_send()
            group(m, HALF - 1, us_sem, ur_sem, to_sib).wait_send()
            return 0
        lax.fori_loop(0, here, sent_rows, 0)

    def spread(packed, out, groups):
        for g in groups:
            val = jnp.sum(jnp.where(lane == g, packed, 0.0), axis=1, keepdims=True)
            out[g * SUB:(g + 1) * SUB] = jnp.broadcast_to(val, (SUB, LANES))

    def gather_rows(reduce, groups):
        packed = jnp.ones((SUB, LANES), F32)
        for g in groups:
            packed = jnp.where(lane == g, reduce(part[g * SUB:(g + 1) * SUB], axis=1, keepdims=True), packed)
        return packed

    def block_at(i):
        return pl.ds(pl.multiple_of(i * RB, RB), RB)

    def m_copy():
        return pltpu.make_async_remote_copy(m_send, m_in, ms_sem, mr_sem, device_id=to_col)

    def cost_min():
        def body(i, _):
            at = block_at(i)
            a_rows = a_rep[at]
            low = None
            for t in range(tiles):
                val = (a_rows + b_ref[:, lanes(t)]) - 2.0 * acc[at, lanes(t)]
                acc[at, lanes(t)] = val
                low = val if low is None else jnp.minimum(low, val)
            part[at] = low
            return 0
        lax.fori_loop(0, blocks, body, 0)
        m_send[...] = gather_rows(jnp.min, range(groups))
        m_copy().start()
        spread(m_send[...], u_rep, range(groups))

    def gibbs(scale):
        def body(i, _):
            at = block_at(i)
            low = u_rep[at]
            total = None
            for t in range(tiles):
                val = jnp.exp((low - acc[at, lanes(t)]) * scale)
                acc[at, lanes(t)] = val
                total = val if total is None else total + val
            part[at] = total
            return 0
        lax.fori_loop(0, blocks, body, 0)
        m_copy().wait()
        f_ref[...] = jnp.exp((jnp.minimum(m_send[...], m_in[...]) - m_send[...]) * scale)

    def row_pass(first_block, last_block, first_tile, last_tile):
        def body(i, _):
            at = block_at(i)
            total = part[at] if first_tile else None
            for t in range(first_tile, last_tile):
                val = acc[at, lanes(t)] * v_ref[:, lanes(t)]
                total = val if total is None else total + val
            part[at] = total
            return 0
        lax.fori_loop(first_block, last_block, body, 0)

    def col_pass(first_block, last_block, half, first):
        mine = range(half * tiles // 2, (half + 1) * tiles // 2)

        def body(i, sums):
            reps = [u_rep[pl.ds(pl.multiple_of(i * RB + k * SUB, SUB), SUB)] for k in range(per)]
            out = []
            for t, val in zip(mine, sums):
                for k in range(per):
                    val = val + acc[pl.ds(pl.multiple_of(i * RB + k * SUB, SUB), SUB), lanes(t)] * reps[k]
                out.append(val)
            return tuple(out)
        start = tuple(jnp.zeros((SUB, LANES), F32) if first else c_part[:, lanes(t)] for t in mine)
        return lax.fori_loop(first_block, last_block, body, start)

    def r_copy(slot, half):
        return pltpu.make_async_remote_copy(r_send.at[slot, half], r_in.at[slot, half], rs_sem.at[slot, half], rr_sem.at[slot, half], device_id=to_col)

    def c_copies(slot, half):
        return [
            pltpu.make_async_remote_copy(c_send.at[slot, half], c_in.at[slot, half, n], cs_sem.at[slot, half, n], cr_sem.at[slot, half, n], device_id=dev)
            for n, dev in enumerate(trio)
        ]

    mid_group, mid_block, mid_col = groups // 2, blocks // 2, cols // 2

    def send_rows(slot, half):
        r_send[slot, half] = gather_rows(jnp.sum, range(half * mid_group, (half + 1) * mid_group)) * f_ref[...]
        r_copy(slot, half).start()

    def take_rows(slot, half):
        r_copy(slot, half).wait_recv()
        u = p_ref[...] / (r_send[slot, half] + r_in[slot, half])
        spread(u * f_ref[...], u_rep, range(half * mid_group, (half + 1) * mid_group))

    def send_cols(slot, half, sums):
        for t, val in enumerate(sums):
            c_send[slot, half, :, lanes(t)] = jnp.sum(val, axis=0, keepdims=True)
        for copy in c_copies(slot, half):
            copy.start()

    def take_cols(slot, half):
        for copy in c_copies(slot, half):
            copy.wait_recv()
        at = slice(half * mid_col, (half + 1) * mid_col)
        total = (c_send[slot, half] + c_in[slot, half, 0]) + (c_in[slot, half, 1] + c_in[slot, half, 2])
        v_ref[:, at] = q_ref[:, at] / total

    def sent(slot):
        for half in range(2):
            r_copy(slot, half).wait_send()
            for copy in c_copies(slot, half):
                copy.wait_send()

    def make_plan():
        def chunk(j, _):
            def body(i, _):
                at = block_at(i)
                for t in range(W // LANES):
                    where = pl.ds(pl.multiple_of(j * W + t * LANES, LANES), LANES)
                    val = (u_rep[at] * acc[at, where]) * v_ref[:, where]
                    acc[at, where] = val
                    panel[j, pl.ds(pl.multiple_of(row_at * rows + i * RB, RB), RB), lanes(t)] = val.astype(BF16)
                return 0
            lax.fori_loop(0, blocks, body, 0)

            @pl.when(j < AHEAD)
            def _():
                issue(j)
            return 0
        lax.fori_loop(0, chunks, chunk, 0)

    def sinkhorn(r):
        cost_min()
        gibbs(1.0 / eps_ref[r])

        def sweep(s, _):
            slot = s % 2

            @pl.when(s == 0)
            def _():
                send_rows(slot, 0)
                send_rows(slot, 1)

            @pl.when(s > 0)
            def _():
                take_cols(1 - slot, 0)
                row_pass(0, mid_block, 0, tiles // 2)
                take_cols(1 - slot, 1)
                row_pass(0, mid_block, tiles // 2, tiles)
                send_rows(slot, 0)
                row_pass(mid_block, blocks, 0, tiles)
                send_rows(slot, 1)

            take_rows(slot, 0)
            for half in range(2):
                for t, val in enumerate(col_pass(0, mid_block, half, True)):
                    c_part[:, lanes(half * tiles // 2 + t)] = val
            take_rows(slot, 1)
            for half in range(2):
                send_cols(slot, half, col_pass(mid_block, blocks, half, False))

            @pl.when(s > 0)
            def _():
                sent(1 - slot)
            return 0
        lax.fori_loop(0, SWEEPS, sweep, 0)
        final = (SWEEPS - 1) % 2
        for half in range(2):
            take_cols(final, half)
        sent(final)
        make_plan()

    def stage_copy(i):
        return pltpu.make_async_copy(t_out.at[pl.ds(pl.multiple_of(i * SUB, SUB), SUB)], stage.at[i % 2], st_sem.at[i % 2])

    def loss():
        stage_copy(0).start()

        def body(g, total):
            @pl.when(g + 1 < groups)
            def _():
                stage_copy(g + 1).start()
            stage_copy(g).wait()
            at = pl.ds(pl.multiple_of(g * SUB, SUB), SUB)
            a_rows = a_rep[at]
            out = None
            for t in range(tiles):
                val = ((a_rows + b_ref[:, lanes(t)]) - 2.0 * acc[at, lanes(t)]) * stage[g % 2, :, lanes(t)]
                out = val if out is None else out + val
            return total + out
        total = lax.fori_loop(0, groups, body, jnp.zeros((SUB, LANES), F32))
        c_send[0, 0, :, lanes(0)] = jnp.sum(total, axis=0, keepdims=True)
        for copy in c_copies(0, 0):
            copy.start()
        for copy in c_copies(0, 0):
            copy.wait()
        total = (c_send[0, 0] + c_in[0, 0, 0]) + (c_in[0, 0, 1] + c_in[0, 0, 2])
        m_send[...] = jnp.broadcast_to(total[:, lanes(0)], (SUB, LANES))
        m_copy().start()
        m_copy().wait()
        loss_out[...] = m_send[...] + m_in[...]

    for j in range(chunks):
        pltpu.make_async_copy(t0_ref.at[:, j * W:(j + 1) * W], panel.at[j, rows_of(row_at)], io_sem).start()
    first_plan = pltpu.make_async_copy(panel.at[:, rows_of(row_at)], panel.at[:, rows_of(row_at)], io_sem)
    width = c1_blk.shape[1]
    c1_at = c1_ref.at[:, pl.ds(pl.multiple_of(col_at * width, width), width)]
    c1_here = pltpu.make_async_copy(c1_blk, c1_at, st_sem.at[0])
    c1_here.start()
    c1_copy = pltpu.make_async_remote_copy(c1_blk, c1_at, os_sem, or_sem, device_id=to_col)
    c1_copy.start()
    own_rows = c2_ref.at[:, pl.ds(pl.multiple_of(row_at * held, held), held)]
    own_block = pltpu.make_async_remote_copy(own_rows, own_rows, bs_sem, br_sem, device_id=to_sib)
    for n in range(chunks):
        piece = c2_blk.at[:, n * W:(n + 1) * W]
        pltpu.make_async_remote_copy(piece, own_rows.at[n], bs_sem, br_sem, device_id=to_sib).start()
    first_plan.wait()
    for j in range(AHEAD):
        issue(j)

    m_send[...] = a_ref[...]
    a_copy = pltpu.make_async_remote_copy(m_send, m_in, ms_sem, mr_sem, device_id=to_col)
    a_copy.start()
    for half in range(2):
        c_send[0, half] = b_part[:, half * mid_col:(half + 1) * mid_col]
        for copy in c_copies(0, half):
            copy.start()
    a_copy.wait()
    spread(m_send[...] + m_in[...], a_rep, range(groups))
    for half in range(2):
        for copy in c_copies(0, half):
            copy.wait()
        total = (c_send[0, half] + c_in[0, half, 0]) + (c_in[0, half, 1] + c_in[0, half, 2])
        b_ref[:, half * mid_col:(half + 1) * mid_col] = total
    c1_here.wait()
    plan_out = pltpu.make_async_copy(acc, t_out, io_sem)
    first_cost(own_block, c1_copy)

    def outer(r, _):
        sinkhorn(r)

        @pl.when(r == steps - 1)
        def _():
            plan_out.start()
            plan_out.wait()
        cost()
        return 0
    lax.fori_loop(0, steps, outer, 0)
    loss()


def packed_rows(vec):
    groups = vec.shape[0] // SUB
    return jnp.pad(vec.reshape(groups, SUB).T, ((0, 0), (0, LANES - groups)), constant_values=1.0)


def solution(mesh):
    grid_spec = P(("pairs", "rows"), "cols")

    def local_fn(c1_blk, c2_blk, t0_blk, p_blk, q_blk, eps_blk):
        col_pos = lax.axis_index("cols")
        row_pos = lax.axis_index("rows")
        c1_width = c1_blk.shape[1]
        c2_height = c2_blk.shape[0]
        rows, cols = t0_blk.shape
        chunks = cols // W
        steps = eps_blk.shape[0]
        p_full = lax.all_gather(p_blk, "rows", tiled=True)
        q_full = lax.all_gather(q_blk, "cols", tiled=True)
        p_piece = lax.dynamic_slice_in_dim(p_full, col_pos * c1_width, c1_width)
        q_piece = lax.dynamic_slice_in_dim(q_full, row_pos * c2_height, c2_height)
        row_term = jnp.sum(c1_blk * c1_blk * p_piece[None, :], axis=1)
        col_term = jnp.sum(c2_blk * c2_blk * q_piece[:, None], axis=0)

        vmem = pl.BlockSpec(memory_space=pltpu.VMEM)
        smem = pl.BlockSpec(memory_space=pltpu.SMEM)
        hbm = pl.BlockSpec(memory_space=pl.ANY)
        dma = pltpu.SemaphoreType.DMA
        plan, loss_part, _, _ = pl.pallas_call(
            functools.partial(outer_kernel, steps),
            out_shape=(
                jax.ShapeDtypeStruct((rows, cols), F32), jax.ShapeDtypeStruct((SUB, LANES), F32),
                jax.ShapeDtypeStruct((chunks, 2 * cols, W), BF16), jax.ShapeDtypeStruct((chunks, cols, W), BF16),
            ),
            in_specs=[hbm, hbm, hbm, vmem, vmem, vmem, vmem, smem],
            out_specs=(hbm, vmem, hbm, hbm),
            scratch_shapes=[
                pltpu.VMEM((rows, cols), F32),
                pltpu.VMEM((chunks, 4 * rows, W), BF16),
                pltpu.VMEM((rows, 4 * rows), BF16),
                pltpu.VMEM((chunks, rows, W), BF16),
                pltpu.VMEM((2, W, cols), BF16),
                pltpu.VMEM((2, W, cols), BF16),
                pltpu.VMEM((HALF - 1, W, W), BF16),
                pltpu.VMEM((HALF - 1, W, W), BF16),
                pltpu.VMEM((1, cols), F32),
                pltpu.VMEM((1, cols), F32),
                *[pltpu.VMEM((rows, LANES), F32)] * 3,
                pltpu.VMEM((SUB, cols), F32),
                pltpu.VMEM((SUB, LANES), F32),
                pltpu.VMEM((SUB, LANES), F32),
                pltpu.VMEM((SUB, LANES), F32),
                pltpu.VMEM((2, 2, SUB, LANES), F32),
                pltpu.VMEM((2, 2, SUB, LANES), F32),
                pltpu.VMEM((2, 2, 1, cols // 2), F32),
                pltpu.VMEM((2, 2, 3, 1, cols // 2), F32),
                pltpu.VMEM((2, SUB, cols), F32),
                *[dma((chunks + 1,))] * 8,
                dma((2,)), dma((2,)), dma, dma, dma((2, 2)), dma((2, 2)), dma((2, 2, 3)), dma((2, 2, 3)),
                dma, dma((2,)),
                *[dma((c2_height // W,))] * 8,
                dma, dma, dma, dma, dma((2,)),
            ],
            compiler_params=pltpu.CompilerParams(collective_id=0, has_side_effects=True, vmem_limit_bytes=67043328),
        )(c1_blk.astype(BF16), t0_blk.astype(BF16), c2_blk.astype(BF16), packed_rows(row_term), col_term[None], packed_rows(p_blk), q_blk[None], eps_blk)
        return plan, jnp.sum(loss_part[0]).reshape(1)

    return jax.shard_map(local_fn, mesh=mesh, in_specs=(grid_spec, grid_spec, grid_spec, P(("pairs", "rows")), P(("pairs", "cols")), P("pairs")), out_specs=(grid_spec, P("pairs")), check_vma=False)
```

```python
import functools

import jax
import jax.numpy as jnp
from jax import lax
from jax.experimental import pallas as pl
from jax.experimental.pallas import tpu as pltpu
from jax.sharding import PartitionSpec as P

SWEEPS = 10
W = 256
AHEAD = 4
RB = 64
HALF = 8
LANES = 128
SUB = 8
F32 = jnp.float32
BF16 = jnp.bfloat16


def outer_kernel(steps, c1_blk, t0_ref, c2_blk, c2_wide, a_ref, q_pack, p_ref, q_ref, eps_ref, t_out, loss_out, c2_ref, c2_turn,
                 acc, panel, c1_ref, lead_in, c2_own, c2_in, turn_in, turn_out, q_in, q_rows, b_ref, v_ref, a_rep, u_rep, part, c_part, f_ref,
                 m_send, m_in, r_send, r_in, c_send, c_in, stage,
                 x_send, x_recv, d_send, d_recv, f_send, f_recv, y_send, y_recv,
                 own_sem, in_sem, ms_sem, mr_sem, rs_sem, rr_sem, cs_sem, cr_sem, io_sem, st_sem,
                 xs_sem, xr_sem, ts_sem, tr_sem, fs_sem, fr_sem, us_sem, ur_sem, bs_sem, br_sem, os_sem, or_sem, qs_sem, qr_sem, turn_sem):
    rows, cols = acc.shape
    chunks = cols // W
    row_at = lax.axis_index("rows")
    col_at = lax.axis_index("cols")
    chip, core = row_at // 2, row_at % 2
    sib = chip * 2 + (1 - core)
    across = (1 - chip) * 2 + core
    diag = (1 - chip) * 2 + (1 - core)
    to_sib, to_across, to_diag, to_col = {"rows": sib}, {"rows": across}, {"rows": diag}, {"cols": 1 - col_at}
    trio = (to_sib, to_across, to_diag)

    barrier = pltpu.get_barrier_semaphore()
    for dev in (*trio, to_col):
        pl.semaphore_signal(barrier, inc=1, device_id=dev)
    pl.semaphore_wait(barrier, 4)

    def rows_of(owner):
        return pl.ds(pl.multiple_of(owner * rows, rows), rows)

    def lead_at(j):
        return panel.at[j, rows_of(sib)]

    last = chunks - 1
    halves = (0, 1)

    def cut(owner, j, half):
        if half is None:
            return panel.at[j, rows_of(owner)], j
        return panel.at[last, rows_of(owner), half * LANES:(half + 1) * LANES], last + half

    def x_copy(j, half=None):
        piece, n = cut(row_at, j, half)
        return pltpu.make_async_remote_copy(piece, piece, x_send.at[n], x_recv.at[n], device_id=to_across)

    def d_copy(j, half=None):
        piece, n = cut(row_at, j, half)
        return pltpu.make_async_remote_copy(piece, piece, d_send.at[n], d_recv.at[n], device_id=to_sib)

    def f_copy(j, half=None):
        piece, n = cut(across, j, half)
        return pltpu.make_async_remote_copy(piece, piece, f_send.at[n], f_recv.at[n], device_id=to_sib)

    def y_copy(j, half=None):
        piece, n = cut(sib, j, half)
        dst = lead_in.at[j] if half is None else lead_in.at[last, :, half * LANES:(half + 1) * LANES]
        return pltpu.make_async_remote_copy(piece, dst, y_send.at[n], y_recv.at[n], device_id=to_col)

    held = c2_blk.shape[0]
    here = held // W

    def wide(n):
        return pl.ds(pl.multiple_of(n * W, W), W)

    def c2_start(owner, i, buf, sem):
        block = owner * (chunks // here) + i // here

        @pl.when(block == row_at)
        def _():
            pltpu.make_async_copy(c2_blk.at[wide(i % here)], buf.at[i % 2], sem.at[i % 2]).start()

        @pl.when(block != row_at)
        def _():
            for n in range(chunks):
                pltpu.make_async_copy(c2_ref.at[n, wide(owner * chunks + i)], buf.at[i % 2, :, n * W:(n + 1) * W], sem.at[i % 2]).start()

    def c2_wait(i, buf, sem):
        pltpu.make_async_copy(c2_blk.at[0:W], buf.at[i % 2], sem.at[i % 2]).wait()

    def add_product(left, right, first):
        tile = 512

        def body(n, _):
            at = pl.ds(pl.multiple_of(n * tile, tile), tile)
            prod = jnp.dot(left[...], right[:, at], preferred_element_type=F32)
            if first:
                acc[:, at] = prod
            else:
                acc[:, at] = acc[:, at] + prod
            return 0
        lax.fori_loop(0, cols // tile, body, 0)

    lane = lax.broadcasted_iota(jnp.int32, (SUB, LANES), 1)

    def lanes(t):
        return slice(t * LANES, (t + 1) * LANES)

    tiles = cols // LANES
    per = RB // SUB
    blocks = rows // RB
    groups = rows // SUB

    def issue(j):
        x_copy(j).start()
        d_copy(j).start()

    def product(owner, i, left, buf, sem, first=False):
        c2_wait(i, buf, sem)
        add_product(left, buf.at[i % 2], first)

        @pl.when(i + 2 < chunks)
        def _():
            c2_start(owner, i + 2, buf, sem)

    def take_chunk(j):
        x_copy(j).wait_recv()
        f_copy(j).start()

        @pl.when(j + AHEAD < last)
        def _():
            issue(j + AHEAD)

        @pl.when(j + AHEAD == last)
        def _():
            for half in halves:
                x_copy(last, half).start()
                d_copy(last, half).start()

    def form_lead(j):
        d_copy(j).wait_recv()
        f_copy(j).wait_recv()
        panel[j, rows_of(sib)] = jnp.dot(c1_ref[...], panel[j], preferred_element_type=F32).astype(BF16)
        y_copy(j).start()

    def last_chunk(between):
        for half, meanwhile in zip(halves, between):
            x_copy(last, half).wait_recv()
            f_copy(last, half).start()
            meanwhile()
            d_copy(last, half).wait_recv()
            f_copy(last, half).wait_recv()
            cols_of = slice(half * LANES, (half + 1) * LANES)
            panel[last, rows_of(sib), cols_of] = jnp.dot(c1_ref[...], panel[last, :, cols_of], preferred_element_type=F32).astype(BF16)
            y_copy(last, half).start()

    def drain_chunks():
        def drain(j, _):
            x_copy(j).wait_send()
            d_copy(j).wait_send()
            f_copy(j).wait_send()
            y_copy(j).wait_send()
            return 0
        lax.fori_loop(0, last, drain, 0)
        for half in halves:
            x_copy(last, half).wait_send()
            d_copy(last, half).wait_send()
            f_copy(last, half).wait_send()
            y_copy(last, half).wait_send()

    plan_out = pltpu.make_async_copy(acc, t_out, io_sem)

    def cost(r):
        for i in range(2):
            c2_start(col_at, i, c2_own, own_sem)
            c2_start(1 - col_at, i, c2_in, in_sem)

        def own_part(i, first=False):
            product(col_at, i, lead_at(i), c2_own, own_sem, first)

        def in_part(i):
            product(1 - col_at, i, lead_in.at[i], c2_in, in_sem)

        def step(j, _):
            take_chunk(j)

            @pl.when((j == 1) & (r == steps - 1))
            def _():
                plan_out.wait()

            @pl.when(j == 1)
            def _():
                own_part(0, True)

            @pl.when(j > 1)
            def _():
                own_part(j - 1)

            form_lead(j)

            @pl.when(j >= 2)
            def _():
                y_copy(j - 2).wait_recv()
                in_part(j - 2)
            return 0
        lax.fori_loop(0, last, step, 0)

        def tail(i, _):
            y_copy(i).wait_recv()
            in_part(i)
            return 0

        last_chunk((lambda: own_part(last - 1), lambda: tail(last - 2, 0)))
        own_part(last)
        tail(last - 1, 0)
        for half in halves:
            y_copy(last, half).wait_recv()
        in_part(last)
        drain_chunks()

    far = 1 - chip

    def quad_rows(base, k):
        return pl.ds(pl.multiple_of(base + k * W, W), W)

    def many(ref, count):
        return ref.at[pl.ds(0, count), pl.ds(0, W)]

    def own_piece(n, m):
        return c2_blk.at[wide(m), wide(n)]

    def sends(src, dst, dst_base, k, m, offsets, sem_s, sem_r, dev):
        for d in offsets:
            n = (k + d) % chunks
            to = dst.at[n, quad_rows(dst_base, m)]
            pltpu.make_async_remote_copy(own_piece(n, m) if src is None else src.at[n, quad_rows(dst_base, m)], to,
                                         sem_s.at[m], sem_r.at[m], device_id=dev).start()

    def group(m, count, sem_s, sem_r, dev):
        return pltpu.make_async_remote_copy(many(c2_ref, count), many(c2_ref, count), sem_s.at[m], sem_r.at[m], device_id=dev)

    straight, turned = range(HALF + 1), range(1, HALF)
    across_base, turn_base = across * held, core * held

    def row_send(m):
        k = core * here + m
        sends(None, c2_ref, row_at * held, k, m, straight, xs_sem, xr_sem, to_across)
        sends(None, c2_turn, turn_base, k, m, turned, ts_sem, tr_sem, to_col)

    def row_forward(m):
        k = core * here + m
        group(m, HALF + 1, xs_sem, xr_sem, to_across).wait_recv()
        sends(c2_ref, c2_ref, across_base, k, m, straight, fs_sem, fr_sem, to_sib)
        group(m, HALF - 1, ts_sem, tr_sem, to_col).wait_recv()
        sends(c2_turn, c2_turn, turn_base, k, m, turned, us_sem, ur_sem, to_sib)

    def row_turn(k):
        def load(src, base):
            for d in turned:
                pltpu.make_async_copy(src.at[(k + d) % chunks, quad_rows(base, k)], turn_in.at[d - 1], turn_sem.at[0]).start()

        @pl.when(chip == col_at)
        def _():
            load(c2_turn, 0)

        @pl.when(chip != col_at)
        def _():
            load(c2_ref, far * cols)
        pltpu.make_async_copy(many(c2_ref, HALF - 1), turn_in, turn_sem.at[0]).wait()
        for d in turned:
            turn_out[d - 1] = turn_in[d - 1].T
        for d in turned:
            pltpu.make_async_copy(turn_out.at[d - 1], c2_ref.at[k, quad_rows(far * cols, (k + d) % chunks)], turn_sem.at[1]).start()
        pltpu.make_async_copy(turn_out, many(c2_ref, HALF - 1), turn_sem.at[1]).wait()

    def col_terms(j):
        count = held // SUB // chunks

        def wide_copy(n):
            src = c2_wide.at[pl.ds(pl.multiple_of((j * count + n) * SUB, SUB), SUB)]
            return pltpu.make_async_copy(src, stage.at[n % 2], st_sem.at[n % 2])
        wide_copy(0).start()

        def body(n, _):
            @pl.when(n + 1 < count)
            def _():
                wide_copy(n + 1).start()
            g = j * count + n
            weight = jnp.sum(jnp.where(lane == g % LANES, q_rows[g // LANES], 0.0), axis=1, keepdims=True)
            weight = jnp.broadcast_to(weight, (SUB, LANES))
            wide_copy(n).wait()
            for t in range(tiles):
                val = stage[n % 2, :, lanes(t)]
                c_part[:, lanes(t)] = c_part[:, lanes(t)] + val * val * weight
            return 0
        lax.fori_loop(0, count, body, 0)

    def first_cost(own_block, c1_copy):
        own_block.wait_recv()
        for i in range(2):
            c2_start(chip, i, c2_own, own_sem)

        def step(j, _):
            @pl.when((j < chunks) & (j % 2 == 0))
            def _():
                row_send(j // 2)

            @pl.when(j < last)
            def _():
                take_chunk(j)

            @pl.when((j == 1) & (chip == col_at))
            def _():
                product(chip, 0, lead_at(0), c2_own, own_sem, True)

            @pl.when((j > 1) & (j <= chunks) & (chip == col_at))
            def _():
                product(chip, j - 1, lead_at(j - 1), c2_own, own_sem)

            @pl.when(j == 0)
            def _():
                c1_copy.wait_recv()

            @pl.when(j < last)
            def _():
                form_lead(j)

            @pl.when(j == last)
            def _():
                last_chunk((lambda: None,) * 2)

            @pl.when(j < chunks)
            def _():
                col_terms(j)

            @pl.when((j >= 2) & (j - 2 < last))
            def _():
                y_copy(j - 2).wait_recv()

            @pl.when(j - 2 == last)
            def _():
                for half in halves:
                    y_copy(last, half).wait_recv()

            @pl.when((j == 2) & (chip != col_at))
            def _():
                product(chip, 0, lead_in.at[0], c2_own, own_sem, True)

            @pl.when((j > 2) & (chip != col_at))
            def _():
                product(chip, j - 2, lead_in.at[j - 2], c2_own, own_sem)

            @pl.when((j > 2) & (j % 2 == 1))
            def _():
                m = (j - 3) // 2
                row_forward(m)
                row_turn(core * here + m)
                group(m, HALF + 1, fs_sem, fr_sem, to_sib).wait_recv()
                group(m, HALF - 1, us_sem, ur_sem, to_sib).wait_recv()
                row_turn((1 - core) * here + m)
            return 0
        lax.fori_loop(0, chunks + 2, step, 0)

        for i in range(2):
            c2_start(far, i, c2_in, in_sem)
        for half in range(2):
            for t in range(tiles // 2):
                c_send[1, half, :, lanes(t)] = jnp.sum(c_part[:, lanes(half * tiles // 2 + t)], axis=0, keepdims=True)
            for copy in c_copies(1, half):
                copy.start()

        def rest(i, _):
            @pl.when(chip == col_at)
            def _():
                product(far, i, lead_in.at[i], c2_in, in_sem)

            @pl.when(chip != col_at)
            def _():
                product(far, i, lead_at(i), c2_in, in_sem)
            return 0
        lax.fori_loop(0, chunks, rest, 0)
        for half in range(2):
            for copy in c_copies(1, half):
                copy.wait()
            total = (c_send[1, half] + c_in[1, half, 0]) + (c_in[1, half, 1] + c_in[1, half, 2])
            b_ref[:, half * mid_col:(half + 1) * mid_col] = total
        drain_chunks()
        own_block.wait_send()
        c1_copy.wait_send()

        def sent_rows(m, _):
            group(m, HALF + 1, xs_sem, xr_sem, to_across).wait_send()
            group(m, HALF - 1, ts_sem, tr_sem, to_col).wait_send()
            group(m, HALF + 1, fs_sem, fr_sem, to_sib).wait_send()
            group(m, HALF - 1, us_sem, ur_sem, to_sib).wait_send()
            return 0
        lax.fori_loop(0, here, sent_rows, 0)

    def spread(packed, out, groups):
        for g in groups:
            val = jnp.sum(jnp.where(lane == g, packed, 0.0), axis=1, keepdims=True)
            out[g * SUB:(g + 1) * SUB] = jnp.broadcast_to(val, (SUB, LANES))

    def gather_rows(reduce, groups):
        packed = jnp.ones((SUB, LANES), F32)
        for g in groups:
            packed = jnp.where(lane == g, reduce(part[g * SUB:(g + 1) * SUB], axis=1, keepdims=True), packed)
        return packed

    def block_at(i):
        return pl.ds(pl.multiple_of(i * RB, RB), RB)

    def m_copy():
        return pltpu.make_async_remote_copy(m_send, m_in, ms_sem, mr_sem, device_id=to_col)

    def cost_min():
        def body(i, _):
            at = block_at(i)
            a_rows = a_rep[at]
            low = None
            for t in range(tiles):
                val = (a_rows + b_ref[:, lanes(t)]) - 2.0 * acc[at, lanes(t)]
                acc[at, lanes(t)] = val
                low = val if low is None else jnp.minimum(low, val)
            part[at] = low
            return 0
        lax.fori_loop(0, blocks, body, 0)
        m_send[...] = gather_rows(jnp.min, range(groups))
        m_copy().start()
        spread(m_send[...], u_rep, range(groups))

    def gibbs(scale):
        def body(i, _):
            at = block_at(i)
            low = u_rep[at]
            total = None
            for t in range(tiles):
                val = jnp.exp((low - acc[at, lanes(t)]) * scale)
                acc[at, lanes(t)] = val
                total = val if total is None else total + val
            part[at] = total
            return 0
        lax.fori_loop(0, blocks, body, 0)
        m_copy().wait()
        f_ref[...] = jnp.exp((jnp.minimum(m_send[...], m_in[...]) - m_send[...]) * scale)

    def row_pass(first_block, last_block, first_tile, last_tile):
        def body(i, _):
            at = block_at(i)
            total = part[at] if first_tile else None
            for t in range(first_tile, last_tile):
                val = acc[at, lanes(t)] * v_ref[:, lanes(t)]
                total = val if total is None else total + val
            part[at] = total
            return 0
        lax.fori_loop(first_block, last_block, body, 0)

    def col_pass(first_block, last_block, half, first):
        mine = range(half * tiles // 2, (half + 1) * tiles // 2)

        def body(i, sums):
            reps = [u_rep[pl.ds(pl.multiple_of(i * RB + k * SUB, SUB), SUB)] for k in range(per)]
            out = []
            for t, val in zip(mine, sums):
                for k in range(per):
                    val = val + acc[pl.ds(pl.multiple_of(i * RB + k * SUB, SUB), SUB), lanes(t)] * reps[k]
                out.append(val)
            return tuple(out)
        start = tuple(jnp.zeros((SUB, LANES), F32) if first else c_part[:, lanes(t)] for t in mine)
        return lax.fori_loop(first_block, last_block, body, start)

    def r_copy(slot, half):
        return pltpu.make_async_remote_copy(r_send.at[slot, half], r_in.at[slot, half], rs_sem.at[slot, half], rr_sem.at[slot, half], device_id=to_col)

    def c_copies(slot, half):
        return [
            pltpu.make_async_remote_copy(c_send.at[slot, half], c_in.at[slot, half, n], cs_sem.at[slot, half, n], cr_sem.at[slot, half, n], device_id=dev)
            for n, dev in enumerate(trio)
        ]

    mid_group, mid_block, mid_col = groups // 2, blocks // 2, cols // 2

    def send_rows(slot, half):
        r_send[slot, half] = gather_rows(jnp.sum, range(half * mid_group, (half + 1) * mid_group)) * f_ref[...]
        r_copy(slot, half).start()

    def take_rows(slot, half):
        r_copy(slot, half).wait_recv()
        u = p_ref[...] / (r_send[slot, half] + r_in[slot, half])
        spread(u * f_ref[...], u_rep, range(half * mid_group, (half + 1) * mid_group))

    def send_cols(slot, half, sums):
        for t, val in enumerate(sums):
            c_send[slot, half, :, lanes(t)] = jnp.sum(val, axis=0, keepdims=True)
        for copy in c_copies(slot, half):
            copy.start()

    def take_cols(slot, half):
        for copy in c_copies(slot, half):
            copy.wait_recv()
        at = slice(half * mid_col, (half + 1) * mid_col)
        total = (c_send[slot, half] + c_in[slot, half, 0]) + (c_in[slot, half, 1] + c_in[slot, half, 2])
        v_ref[:, at] = q_ref[:, at] / total

    def sent(slot):
        for half in range(2):
            r_copy(slot, half).wait_send()
            for copy in c_copies(slot, half):
                copy.wait_send()

    def form_chunks(form):
        def chunk(j, _):
            def body(i, _):
                at = block_at(i)
                for t in range(W // LANES):
                    where = pl.ds(pl.multiple_of(j * W + t * LANES, LANES), LANES)
                    panel[j, pl.ds(pl.multiple_of(row_at * rows + i * RB, RB), RB), lanes(t)] = form(at, where).astype(BF16)
                return 0
            lax.fori_loop(0, blocks, body, 0)

            @pl.when(j < AHEAD)
            def _():
                issue(j)
            return 0
        lax.fori_loop(0, chunks, chunk, 0)

    def plan_at(at, where):
        val = (u_rep[at] * acc[at, where]) * v_ref[:, where]
        acc[at, where] = val
        return val

    def sinkhorn(r):
        cost_min()
        gibbs(1.0 / eps_ref[r])

        def sweep(s, _):
            slot = s % 2

            @pl.when(s == 0)
            def _():
                send_rows(slot, 0)
                send_rows(slot, 1)

            @pl.when(s > 0)
            def _():
                take_cols(1 - slot, 0)
                row_pass(0, mid_block, 0, tiles // 2)
                take_cols(1 - slot, 1)
                row_pass(0, mid_block, tiles // 2, tiles)
                send_rows(slot, 0)
                row_pass(mid_block, blocks, 0, tiles)
                send_rows(slot, 1)

            take_rows(slot, 0)
            for half in range(2):
                for t, val in enumerate(col_pass(0, mid_block, half, True)):
                    c_part[:, lanes(half * tiles // 2 + t)] = val
            take_rows(slot, 1)
            for half in range(2):
                send_cols(slot, half, col_pass(mid_block, blocks, half, False))

            @pl.when(s > 0)
            def _():
                sent(1 - slot)
            return 0
        lax.fori_loop(0, SWEEPS, sweep, 0)
        final = (SWEEPS - 1) % 2
        for half in range(2):
            take_cols(final, half)
        sent(final)
        form_chunks(plan_at)

    def stage_copy(i):
        return pltpu.make_async_copy(t_out.at[pl.ds(pl.multiple_of(i * SUB, SUB), SUB)], stage.at[i % 2], st_sem.at[i % 2])

    def loss():
        stage_copy(0).start()

        def body(g, total):
            @pl.when(g + 1 < groups)
            def _():
                stage_copy(g + 1).start()
            stage_copy(g).wait()
            at = pl.ds(pl.multiple_of(g * SUB, SUB), SUB)
            a_rows = a_rep[at]
            out = None
            for t in range(tiles):
                val = ((a_rows + b_ref[:, lanes(t)]) - 2.0 * acc[at, lanes(t)]) * stage[g % 2, :, lanes(t)]
                out = val if out is None else out + val
            return total + out
        total = lax.fori_loop(0, groups, body, jnp.zeros((SUB, LANES), F32))
        c_send[0, 0, :, lanes(0)] = jnp.sum(total, axis=0, keepdims=True)
        for copy in c_copies(0, 0):
            copy.start()
        for copy in c_copies(0, 0):
            copy.wait()
        total = (c_send[0, 0] + c_in[0, 0, 0]) + (c_in[0, 0, 1] + c_in[0, 0, 2])
        m_send[...] = jnp.broadcast_to(total[:, lanes(0)], (SUB, LANES))
        m_copy().start()
        m_copy().wait()
        loss_out[...] = m_send[...] + m_in[...]

    first_plan = pltpu.make_async_copy(t0_ref, acc, io_sem)
    first_plan.start()
    q_copy = pltpu.make_async_remote_copy(q_pack, q_in, qs_sem, qr_sem, device_id=to_col)
    q_copy.start()
    width = c1_blk.shape[1]
    c1_at = c1_ref.at[:, pl.ds(pl.multiple_of(col_at * width, width), width)]
    c1_here = pltpu.make_async_copy(c1_blk, c1_at, st_sem.at[0])
    c1_here.start()
    c1_copy = pltpu.make_async_remote_copy(c1_blk, c1_at, os_sem, or_sem, device_id=to_col)
    c1_copy.start()
    own_rows = c2_ref.at[:, pl.ds(pl.multiple_of(row_at * held, held), held)]
    own_block = pltpu.make_async_remote_copy(own_rows, own_rows, bs_sem, br_sem, device_id=to_sib)
    for n in range(chunks):
        piece = c2_blk.at[:, n * W:(n + 1) * W]
        pltpu.make_async_remote_copy(piece, own_rows.at[n], bs_sem, br_sem, device_id=to_sib).start()
    first_plan.wait()
    form_chunks(lambda at, where: acc[at, where])

    m_send[...] = a_ref[...]
    m_copy().start()
    q_copy.wait()
    for n in range(q_rows.shape[0]):
        piece = pl.ds(pl.multiple_of((core * q_rows.shape[0] + n) * LANES, LANES), LANES)

        @pl.when(chip == col_at)
        def _():
            q_rows[n] = q_pack[:, piece]

        @pl.when(chip != col_at)
        def _():
            q_rows[n] = q_in[:, piece]
    c_part[...] = jnp.zeros_like(c_part)
    m_copy().wait()
    spread(m_send[...] + m_in[...], a_rep, range(groups))
    c1_here.wait()
    first_cost(own_block, c1_copy)

    def outer(r, _):
        sinkhorn(r)

        @pl.when(r == steps - 1)
        def _():
            plan_out.start()
        cost(r)
        return 0
    lax.fori_loop(0, steps, outer, 0)
    loss()


def packed_rows(vec):
    groups = vec.shape[0] // SUB
    return jnp.pad(vec.reshape(groups, SUB).T, ((0, 0), (0, LANES - groups)), constant_values=1.0)


def solution(mesh):
    grid_spec = P(("pairs", "rows"), "cols")

    def local_fn(c1_blk, c2_blk, t0_blk, p_blk, q_blk, eps_blk):
        col_pos = lax.axis_index("cols")
        c1_width = c1_blk.shape[1]
        c2_height = c2_blk.shape[0]
        rows, cols = t0_blk.shape
        chunks = cols // W
        steps = eps_blk.shape[0]
        p_full = lax.all_gather(p_blk, "rows", tiled=True)
        p_piece = lax.dynamic_slice_in_dim(p_full, col_pos * c1_width, c1_width)
        row_term = jnp.sum(c1_blk * c1_blk * p_piece[None, :], axis=1)
        q_pack = q_blk.reshape(cols // SUB, SUB).T

        vmem = pl.BlockSpec(memory_space=pltpu.VMEM)
        smem = pl.BlockSpec(memory_space=pltpu.SMEM)
        hbm = pl.BlockSpec(memory_space=pl.ANY)
        dma = pltpu.SemaphoreType.DMA
        plan, loss_part, _, _ = pl.pallas_call(
            functools.partial(outer_kernel, steps),
            out_shape=(
                jax.ShapeDtypeStruct((rows, cols), F32), jax.ShapeDtypeStruct((SUB, LANES), F32),
                jax.ShapeDtypeStruct((chunks, 2 * cols, W), BF16), jax.ShapeDtypeStruct((chunks, cols, W), BF16),
            ),
            in_specs=[hbm, hbm, hbm, hbm, vmem, vmem, vmem, vmem, smem],
            out_specs=(hbm, vmem, hbm, hbm),
            scratch_shapes=[
                pltpu.VMEM((rows, cols), F32),
                pltpu.VMEM((chunks, 4 * rows, W), BF16),
                pltpu.VMEM((rows, 4 * rows), BF16),
                pltpu.VMEM((chunks, rows, W), BF16),
                pltpu.VMEM((2, W, cols), BF16),
                pltpu.VMEM((2, W, cols), BF16),
                pltpu.VMEM((HALF - 1, W, W), BF16),
                pltpu.VMEM((HALF - 1, W, W), BF16),
                pltpu.VMEM((SUB, cols // SUB), F32),
                pltpu.VMEM((c2_height // SUB // LANES, SUB, LANES), F32),
                pltpu.VMEM((1, cols), F32),
                pltpu.VMEM((1, cols), F32),
                *[pltpu.VMEM((rows, LANES), F32)] * 3,
                pltpu.VMEM((SUB, cols), F32),
                pltpu.VMEM((SUB, LANES), F32),
                pltpu.VMEM((SUB, LANES), F32),
                pltpu.VMEM((SUB, LANES), F32),
                pltpu.VMEM((2, 2, SUB, LANES), F32),
                pltpu.VMEM((2, 2, SUB, LANES), F32),
                pltpu.VMEM((2, 2, 1, cols // 2), F32),
                pltpu.VMEM((2, 2, 3, 1, cols // 2), F32),
                pltpu.VMEM((2, SUB, cols), F32),
                *[dma((chunks + 1,))] * 8,
                dma((2,)), dma((2,)), dma, dma, dma((2, 2)), dma((2, 2)), dma((2, 2, 3)), dma((2, 2, 3)),
                dma, dma((2,)),
                *[dma((c2_height // W,))] * 8,
                dma, dma, dma, dma, dma, dma, dma((2,)),
            ],
            compiler_params=pltpu.CompilerParams(collective_id=0, has_side_effects=True, vmem_limit_bytes=67043328),
        )(c1_blk.astype(BF16), t0_blk, c2_blk.astype(BF16), c2_blk, packed_rows(row_term), q_pack, packed_rows(p_blk), q_blk[None], eps_blk)
        return plan, jnp.sum(loss_part[0]).reshape(1)

    return jax.shard_map(local_fn, mesh=mesh, in_specs=(grid_spec, grid_spec, grid_spec, P(("pairs", "rows")), P(("pairs", "cols")), P("pairs")), out_specs=(grid_spec, P("pairs")), check_vma=False)
```
